32 devices in a mesh: gy: 8 (over z, core), gz: 4 (over y, x).
Axes of the slice: x: 2, y: 2, z: 4, core: 2. Of those that a mesh axis runs over, the one named last changes fastest.
Arguments:
- phase_field: float32 [128, 512, 1024], P('gz', 'gy'), may hold values from 0 to 1
- others: float32 [128, 512, 1024], P('gz', 'gy'), may hold values from 0 to 1
- cond_x: float32 [1023], replicated, may hold values from 256 to 4096
- cond_y: float32 [511], replicated, may hold values from 256 to 4096
- cond_z: float32 [127], replicated, may hold values from 64 to 1024
- inverse_x: float32 [1024, 1024], replicated, as said below
- inverse_y: float32 [512, 512], replicated
- inverse_z: float32 [128, 128], replicated
Outputs:
- grown: float32 [128, 512, 1024], P('gz', 'gy')
The draws below stay inside these ranges and needn't reach their ends.
Inputs may be any that keep to these rules, and one draw needn't show every extreme that they name: inverse_x is the inverse of the 1024 x 1024 matrix I - 0.5 Lx, where Lx maps a line v to cond_x[i] (v[i+1] - v[i]) - cond_x[i-1] (v[i] - v[i-1]) with the missing edges at the ends left out; inverse_y and inverse_z are built likewise from cond_y and cond_z.
All inputs are finite; a program needn't handle non-finite values.
Results may differ from the reference program's by a relative error of at most 0.0003.
Values sent between devices are 32-bit elements; how exact they have to be, the bound alone decides.
No kernel may reach another device: no remote copies, remote signals or barrier semaphores. Data moves between devices by JAX's collectives and lax.ppermute only.
A program may use at most 128 MiB of HBM per device.

```python
import jax
import jax.numpy as jnp
from jax import lax

NX = 1024
NY = 512
NZ = 128
STEPS = 2


lateral_low = 256.0


lateral_high = 4096.0


growth_low = 64.0


growth_high = 1024.0


def line_system(key, tag, count, low, high):
    sub = jax.random.fold_in(key, tag)
    logs = jax.random.uniform(sub, (count - 1,), jnp.float32, jnp.log(low), jnp.log(high))
    weights = jnp.exp(logs)
    padded = jnp.pad(weights, (1, 1))
    diagonal = 1.0 + 0.5 * (padded[:-1] + padded[1:])
    matrix = jnp.diag(diagonal) - 0.5 * jnp.diag(weights, 1) - 0.5 * jnp.diag(weights, -1)
    inverse = jnp.linalg.solve(matrix, jnp.eye(count, dtype=jnp.float32))
    return (weights, inverse)


def draw_cond_x(key, part):
    return line_system(key, 11, NX, lateral_low, lateral_high)[0]


def draw_inverse_x(key, part):
    return line_system(key, 11, NX, lateral_low, lateral_high)[1]


def draw_cond_y(key, part):
    return line_system(key, 12, NY, lateral_low, lateral_high)[0]


def draw_inverse_y(key, part):
    return line_system(key, 12, NY, lateral_low, lateral_high)[1]


def draw_cond_z(key, part):
    return line_system(key, 13, NZ, growth_low, growth_high)[0]


def draw_inverse_z(key, part):
    return line_system(key, 13, NZ, growth_low, growth_high)[1]


def smooth_part(key):
    keys = jax.random.split(key, 2)
    waves = jax.random.randint(keys[0], (3,), 1, 5).astype(jnp.float32)
    shifts = jax.random.uniform(keys[1], (3,), jnp.float32, -3.14159, 3.14159)
    coord_z = jnp.arange(NZ, dtype=jnp.float32) / NZ
    coord_y = jnp.arange(NY, dtype=jnp.float32) / NY
    coord_x = jnp.arange(NX, dtype=jnp.float32) / NX
    wave_z = jnp.cos(6.28318 * waves[0] * coord_z + shifts[0])
    wave_y = jnp.cos(6.28318 * waves[1] * coord_y + shifts[1])
    wave_x = jnp.cos(6.28318 * waves[2] * coord_x + shifts[2])
    return wave_z[:, None, None] * wave_y[None, :, None] * wave_x[None, None, :]


def field_draw(key, tag):
    sub = jax.random.fold_in(key, tag)
    first, second = jax.random.split(sub)
    rough = jax.random.uniform(first, (NZ, NY, NX), jnp.float32, 0.0, 1.0)
    smooth = smooth_part(second)
    return 0.5 * rough + 0.25 + 0.25 * smooth


def draw_phase_field(key, part):
    return field_draw(key, 21)


def draw_others(key, part):
    return field_draw(key, 22)


def setup_inputs(seed: int = 0) -> dict:
    arg_keys = jax.random.split(jax.random.key(seed), 9)
    phase_field = draw_phase_field(jax.random.fold_in(arg_keys[8], 71), 0)
    others = draw_others(jax.random.fold_in(arg_keys[8], 71), 0)
    cond_x = draw_cond_x(jax.random.fold_in(arg_keys[8], 71), 0)
    cond_y = draw_cond_y(jax.random.fold_in(arg_keys[8], 71), 0)
    cond_z = draw_cond_z(jax.random.fold_in(arg_keys[8], 71), 0)
    inverse_x = draw_inverse_x(jax.random.fold_in(arg_keys[8], 71), 0)
    inverse_y = draw_inverse_y(jax.random.fold_in(arg_keys[8], 71), 0)
    inverse_z = draw_inverse_z(jax.random.fold_in(arg_keys[8], 71), 0)
    return {"phase_field": phase_field, "others": others, "cond_x": cond_x, "cond_y": cond_y, "cond_z": cond_z, "inverse_x": inverse_x, "inverse_y": inverse_y, "inverse_z": inverse_z}


reaction_rate = 2.0

def laplace(field, cond_x, cond_y, cond_z):
    flux_x = jnp.pad(jnp.diff(field, axis=2) * cond_x, ((0, 0), (0, 0), (1, 1)))
    flux_y = jnp.pad(jnp.diff(field, axis=1) * cond_y[:, None], ((0, 0), (1, 1), (0, 0)))
    flux_z = jnp.pad(jnp.diff(field, axis=0) * cond_z[:, None, None], ((1, 1), (0, 0), (0, 0)))
    total = flux_x[:, :, 1:] - flux_x[:, :, :-1]
    total = total + (flux_y[:, 1:, :] - flux_y[:, :-1, :])
    return total + (flux_z[1:] - flux_z[:-1])

def reference(phase_field, others, cond_x, cond_y, cond_z, inverse_x, inverse_y, inverse_z):
    field = phase_field
    for step in range(STEPS):
        lap = laplace(field, cond_x, cond_y, cond_z)
        rhs = lap + reaction_rate * (field - field * field * field - 2.0 * field * others)
        moved = jnp.einsum('zyx,wx->zyw', rhs, inverse_x, precision=lax.Precision.HIGHEST)
        moved = jnp.einsum('zyx,wy->zwx', moved, inverse_y, precision=lax.Precision.HIGHEST)
        moved = jnp.einsum('zyx,wz->wyx', moved, inverse_z, precision=lax.Precision.HIGHEST)
        field = field + moved
    return field
```

```python
import functools

import jax
import jax.numpy as jnp
from jax import lax
from jax.experimental import pallas as pl
from jax.experimental.pallas import tpu as pltpu
from jax.sharding import PartitionSpec as P

STEPS = 2
REACTION = 2.0
LANES = 128
SUB = 8
XB = 256
ZB = 8

f32 = jnp.float32
bf16 = jnp.bfloat16


def halves(a):
    high = lax.reduce_precision(a, 8, 7)
    low = a - high
    return high.astype(bf16), low.astype(bf16)


def split(a):
    high = a.astype(bf16)
    low = (a - high.astype(f32)).astype(bf16)
    return high, low


def wide(column, lanes=LANES):
    return jnp.broadcast_to(column[:, None], (column.shape[0], lanes))


def line_tables(inverse, axis, count):
    total = inverse.shape[0]
    parts = lax.axis_size(axis)
    me = lax.axis_index(axis)
    start = me * count
    before = jnp.maximum(start - 1, 0)
    after = jnp.minimum(start + count, total - 1)
    block = lax.dynamic_slice(inverse, (start, start), (count, count))
    eye = jnp.eye(count, dtype=f32)
    diag = jnp.sum(block * eye, axis=0)
    column = lax.dynamic_slice(inverse, (start, before), (count, 1))[:, 0]
    pivot = lax.dynamic_slice(inverse, (before, before), (1, 1))[0, 0]
    from_low = column / pivot
    column = lax.dynamic_slice(inverse, (start, after), (count, 1))[:, 0]
    pivot = lax.dynamic_slice(inverse, (after, after), (1, 1))[0, 0]
    from_high = column / pivot
    lasts = inverse[count - 1 :: count, count - 1 :: count]
    firsts = inverse[::count, ::count]
    unit = jnp.eye(parts, dtype=f32)
    carry_up = lasts / jnp.sum(lasts * unit, axis=0)[None, :]
    carry_down = firsts / jnp.sum(firsts * unit, axis=0)[None, :]
    return dict(
        block=block,
        diag=diag,
        from_low=from_low,
        from_high=from_high,
        carry_up=carry_up,
        carry_down=carry_down,
    )


def entry(table, i, j):
    n = table.shape[0]
    i = jnp.clip(i, 0, n - 1)
    j = jnp.clip(j, 0, n - 1)
    return lax.dynamic_slice(table, (i, j), (1, 1))[0, 0]


def cyclic(size, k, stride=1):
    groups = size // stride
    return [
        (c * stride + r, ((c + k) % groups) * stride + r)
        for c in range(groups)
        for r in range(stride)
    ]


def carries_direct(up, down, tables, axis):
    parts = lax.axis_size(axis)
    me = lax.axis_index(axis)
    low = jnp.zeros_like(up)
    high = jnp.zeros_like(up)
    got = []
    for k in range(1, parts):
        dest = (me + k) % parts
        got.append(lax.ppermute(jnp.where(dest > me, up, down), axis, cyclic(parts, k)))
    for k in range(1, parts):
        src = (me - k) % parts
        below = src < me
        a = jnp.where(below, entry(tables["carry_up"], me - 1, src), 0.0)
        b = jnp.where(below, 0.0, entry(tables["carry_down"], me + 1, src))
        low = low + a * got[k - 1]
        high = high + b * got[k - 1]
    return low, high


def carries_paired(both, tables, axis):
    parts = lax.axis_size(axis)
    me = lax.axis_index(axis)
    chips = parts // 2
    core = me % 2
    chip = me // 2
    half = both.shape[1] // 2
    up_t, down_t = tables["carry_up"], tables["carry_down"]
    even, odd = 2 * chip, 2 * chip + 1
    first, second = both[:, :half], both[:, half:]
    mine = jnp.where(core == 0, first, second)
    theirs = jnp.where(core == 0, second, first)
    swap = [(i, i ^ 1) for i in range(parts)]
    other = lax.ppermute(theirs, axis, swap)
    of_even = jnp.where(core == 0, mine, other)
    of_odd = jnp.where(core == 0, other, mine)
    up = of_odd[0] + entry(up_t, odd, even) * of_even[0]
    down = of_even[1] + entry(down_t, even, odd) * of_odd[1]
    got = []
    for k in range(1, chips):
        dest = (chip + k) % chips
        got.append(
            lax.ppermute(jnp.where(dest > chip, up, down), axis, cyclic(parts, k, 2))
        )
    low = jnp.zeros_like(up)
    high = jnp.zeros_like(up)
    for k in range(1, chips):
        src = (chip - k) % chips
        below = src < chip
        a = jnp.where(below, entry(up_t, even - 1, 2 * src + 1), 0.0)
        b = jnp.where(below, 0.0, entry(down_t, odd + 1, 2 * src))
        low = low + a * got[k - 1]
        high = high + b * got[k - 1]
    odd_low = of_even[0] + jnp.where(chip > 0, entry(up_t, even, even - 1), 0.0) * low
    even_high = (
        of_odd[1] + jnp.where(chip < chips - 1, entry(down_t, odd, odd + 1), 0.0) * high
    )
    for_even = jnp.stack([low, even_high])
    for_odd = jnp.stack([odd_low, high])
    keep = jnp.where(core == 0, for_even, for_odd)
    give = jnp.where(core == 0, for_odd, for_even)
    back = lax.ppermute(give, axis, swap)
    head = jnp.where(core == 0, keep, back)
    tail = jnp.where(core == 0, back, keep)
    whole = jnp.concatenate([head, tail], axis=1)
    return whole[0], whole[1]


def explicit_kernel(
    u_ref, below_ref, above_ref, o_ref, ylo_ref, yhi_ref, zlo_ref, zhi_ref,
    cx_ref, cup_ref, cdn_ref, cz_ref, wz_ref, ay_ref, axh_ref, axl_ref, xlo_ref, xhi_ref,
    t_ref, sy_ref, sz_ref, rhs_ref, line_ref,
):
    step = pl.program_id(0)
    steps = pl.num_programs(0)
    zb, rows, nx = u_ref.shape
    tiles = rows // SUB
    blocks = nx // XB
    sub = lax.broadcasted_iota(jnp.int32, (SUB, nx), 0)
    cx = cx_ref[...]

    def plane(z, carry):
        zz = step * zb + z
        c_up = cz_ref[zz + 1]
        c_dn = cz_ref[zz]

        def get(r):
            return u_ref[z, r * SUB : (r + 1) * SUB, :]

        low_row = ylo_ref[pl.ds(zz, 1), :]
        high_row = yhi_ref[pl.ds(zz, 1), :]
        before = jnp.broadcast_to(low_row, (SUB, nx))
        current = get(0)
        down_roll = pltpu.roll(current, 1, 0)
        for r in range(tiles):
            lane_rows = slice(r * SUB, (r + 1) * SUB)
            if r + 1 < tiles:
                following = get(r + 1)
                up_next = pltpu.roll(following, SUB - 1, 0)
                down_next = pltpu.roll(following, 1, 0)
            else:
                following = None
                up_next = jnp.broadcast_to(high_row, (SUB, nx))
                down_next = None
            c = current
            down = jnp.where(sub == 0, before, down_roll)
            up = jnp.where(sub == SUB - 1, up_next, pltpu.roll(c, SUB - 1, 0))
            fx = (pltpu.roll(c, nx - 1, 1) - c) * cx
            total = fx - pltpu.roll(fx, 1, 1)
            cup = jnp.concatenate([cup_ref[lane_rows, :]] * (nx // LANES), axis=1)
            cdn = jnp.concatenate([cdn_ref[lane_rows, :]] * (nx // LANES), axis=1)
            total = total + ((up - c) * cup - (c - down) * cdn)
            zdn = lax.select(
                z > 0,
                u_ref[jnp.maximum(z - 1, 0), lane_rows, :],
                lax.select(step > 0, below_ref[0, lane_rows, :], zlo_ref[lane_rows, :]),
            )
            zup = lax.select(
                z < zb - 1,
                u_ref[jnp.minimum(z + 1, zb - 1), lane_rows, :],
                lax.select(
                    step < steps - 1, above_ref[0, lane_rows, :], zhi_ref[lane_rows, :]
                ),
            )
            total = total + ((zup - c) * c_up - (c - zdn) * c_dn)
            o = o_ref[z, lane_rows, :]
            total = total + (REACTION * c) * (1.0 - c * c - 2.0 * o)
            rhs_ref[pl.ds(pl.multiple_of(z * rows + r * SUB, SUB), SUB), :] = total
            before = down_roll
            current = following
            down_roll = down_next
        return carry

    lax.fori_loop(0, zb, plane, 0)

    for e in range(blocks):
        cols = slice(e * XB, (e + 1) * XB)
        high, low = split(rhs_ref[:, cols])
        dot = functools.partial(jnp.dot, preferred_element_type=f32)
        line_ref[:, cols] = (
            dot(high, axh_ref[e]) + dot(low, axh_ref[e]) + dot(high, axl_ref[e])
        )
    lows = []
    w = None
    for e in range(blocks):
        end = line_ref[:, (e + 1) * XB - 1 : (e + 1) * XB]
        lows.append(w)
        if w is not None:
            end = end + w * xlo_ref[:, (e + 1) * XB - 1 : (e + 1) * XB]
        w = end
    highs = [None] * blocks
    w = None
    for e in reversed(range(blocks)):
        end = line_ref[:, e * XB : e * XB + 1]
        highs[e] = w
        if w is not None:
            end = end + w * xhi_ref[:, e * XB : e * XB + 1]
        w = end
    for e in range(blocks):
        cols = slice(e * XB, (e + 1) * XB)
        value = line_ref[:, cols]
        if lows[e] is not None:
            value = value + lows[e] * xlo_ref[:, cols]
        if highs[e] is not None:
            value = value + highs[e] * xhi_ref[:, cols]
        line_ref[:, cols] = value

    @pl.when(step == 0)
    def _():
        sz_ref[...] = jnp.zeros_like(sz_ref)

    def solve(z, carry):
        zz = step * zb + z
        base = pl.multiple_of(z * rows, rows)
        high, low = split(line_ref[pl.ds(base, rows), :])
        both = jnp.concatenate([high, low], axis=0)
        result = jnp.dot(ay_ref[...], both, preferred_element_type=f32)
        value = result[:rows] + result[rows:]
        t_ref[z] = value
        sy_ref[0, pl.ds(z, 1), :] = value[rows - 1 :]
        sy_ref[1, pl.ds(z, 1), :] = value[:1]
        sz_ref[0] = sz_ref[0] + wz_ref[0, zz] * value
        sz_ref[1] = sz_ref[1] + wz_ref[1, zz] * value
        return carry

    lax.fori_loop(0, zb, solve, 0)


def explicit(u, o, halos, tabs):
    nz, rows, nx = u.shape
    zb = ZB
    steps = nz // zb
    whole = lambda a: pl.BlockSpec(a.shape, lambda s: (0,) * a.ndim)
    smem = pl.BlockSpec(memory_space=pltpu.SMEM)
    field = pl.BlockSpec((zb, rows, nx), lambda s: (s, 0, 0))
    ylo, yhi, zlo, zhi = halos
    in_arrays = [
        (u, field),
        (u, pl.BlockSpec((1, rows, nx), lambda s: (jnp.maximum(s * zb - 1, 0), 0, 0))),
        (u, pl.BlockSpec((1, rows, nx), lambda s: (jnp.minimum(s * zb + zb, nz - 1), 0, 0))),
        (o, field),
        (ylo, whole(ylo)), (yhi, whole(yhi)), (zlo, whole(zlo)), (zhi, whole(zhi)),
        (tabs["cx"], whole(tabs["cx"])),
        (tabs["cup"], whole(tabs["cup"])),
        (tabs["cdn"], whole(tabs["cdn"])),
        (tabs["cz"], smem),
        (tabs["wz"], smem),
        (tabs["ay"], whole(tabs["ay"])),
        (tabs["axh"], whole(tabs["axh"])),
        (tabs["axl"], whole(tabs["axl"])),
        (tabs["xlo"], whole(tabs["xlo"])),
        (tabs["xhi"], whole(tabs["xhi"])),
    ]
    return pl.pallas_call(
        explicit_kernel,
        grid=(steps,),
        in_specs=[s for _, s in in_arrays],
        out_specs=[
            field,
            pl.BlockSpec((2, zb, nx), lambda s: (0, s, 0)),
            pl.BlockSpec((2, rows, nx), lambda s: (0, 0, 0)),
        ],
        out_shape=[
            jax.ShapeDtypeStruct(u.shape, f32),
            jax.ShapeDtypeStruct((2, nz, nx), f32),
            jax.ShapeDtypeStruct((2, rows, nx), f32),
        ],
        scratch_shapes=[
            pltpu.VMEM((zb * rows, nx), f32),
            pltpu.VMEM((zb * rows, nx), f32),
        ],
        compiler_params=pltpu.CompilerParams(
            dimension_semantics=("arbitrary",), vmem_limit_bytes=48 * 2**20
        ),
        name="explicit",
    )(*[a for a, _ in in_arrays])


def update_kernel(
    t_ref, u_ref, p_ref, q_ref, zl_ref, zr_ref, flo_ref, fhi_ref, coef_ref,
    out_ref, e_ref,
):
    nz, sub, nx = t_ref.shape
    lo = jnp.concatenate([flo_ref[...]] * (nx // LANES), axis=1)
    hi = jnp.concatenate([fhi_ref[...]] * (nx // LANES), axis=1)

    def forward(z, carry):
        v = t_ref[z] + lo * p_ref[pl.ds(z, 1), :] + hi * q_ref[pl.ds(z, 1), :]
        e = coef_ref[0, z] * v
        e_ref[z] = e
        s = carry + e
        out_ref[z] = u_ref[z] + s
        return coef_ref[1, z] * s

    lax.fori_loop(0, nz, forward, coef_ref[3, 0] * zl_ref[...], unroll=4)

    def backward(k, carry):
        z = nz - 1 - k
        out_ref[z] = out_ref[z] + carry
        return coef_ref[2, z] * (carry + e_ref[z])

    lax.fori_loop(0, nz, backward, coef_ref[3, 1] * zr_ref[...], unroll=4)


def update(t, u, p, q, zl, zr, tabs):
    nz, rows, nx = u.shape
    field = pl.BlockSpec((nz, SUB, nx), lambda r: (0, r, 0))
    flat = pl.BlockSpec((nz, nx), lambda r: (0, 0))
    tile = pl.BlockSpec((SUB, nx), lambda r: (r, 0))
    lane = pl.BlockSpec((SUB, LANES), lambda r: (r, 0))
    return pl.pallas_call(
        update_kernel,
        grid=(rows // SUB,),
        in_specs=[
            field, field, flat, flat, tile, tile, lane, lane,
            pl.BlockSpec(memory_space=pltpu.SMEM),
        ],
        out_specs=field,
        out_shape=jax.ShapeDtypeStruct(u.shape, f32),
        scratch_shapes=[pltpu.VMEM((nz, SUB, nx), f32)],
        compiler_params=pltpu.CompilerParams(
            dimension_semantics=("arbitrary",), vmem_limit_bytes=24 * 2**20
        ),
        name="update",
    )(t, u, p, q, zl, zr, tabs["flo"], tabs["fhi"], tabs["coef"])


def halo(u):
    ny, nz = lax.axis_size("gy"), lax.axis_size("gz")
    up = lambda n: [(i, i + 1) for i in range(n - 1)]
    down = lambda n: [(i + 1, i) for i in range(n - 1)]
    ylo = lax.ppermute(u[:, -1, :], "gy", up(ny))
    yhi = lax.ppermute(u[:, 0, :], "gy", down(ny))
    zlo = lax.ppermute(u[-1], "gz", up(nz))
    zhi = lax.ppermute(u[0], "gz", down(nz))
    return ylo, yhi, zlo, zhi


def x_tables(inverse):
    nx = inverse.shape[0]
    blocks = nx // XB
    diag = jnp.stack(
        [inverse[e * XB : (e + 1) * XB, e * XB : (e + 1) * XB].T for e in range(blocks)]
    )
    high, low = halves(diag)
    zero = jnp.zeros((XB,), f32)
    lows, highs = [zero], []
    for e in range(1, blocks):
        c = e * XB - 1
        lows.append(inverse[e * XB : (e + 1) * XB, c] / inverse[c, c])
    for e in range(blocks - 1):
        c = (e + 1) * XB
        highs.append(inverse[e * XB : (e + 1) * XB, c] / inverse[c, c])
    highs.append(zero)
    return high, low, jnp.concatenate(lows)[None], jnp.concatenate(highs)[None]


def body(phase_field, others, cond_x, cond_y, cond_z, inverse_x, inverse_y, inverse_z):
    depth, rows, nx = phase_field.shape
    ty = line_tables(inverse_y, "gy", rows)
    tz = line_tables(inverse_z, "gz", depth)
    y0 = lax.axis_index("gy") * rows
    z0 = lax.axis_index("gz") * depth
    ye = lax.dynamic_slice_in_dim(jnp.pad(cond_y, (1, 1)), y0, rows + 1)
    ze = lax.dynamic_slice_in_dim(jnp.pad(cond_z, (1, 1)), z0, depth + 1)
    axh, axl, xlo, xhi = x_tables(inverse_x)
    ah, al = halves(ty["block"])
    ay = jnp.concatenate(
        [
            jnp.concatenate([ah, ah], axis=1),
            jnp.concatenate([al, jnp.zeros_like(al)], axis=1),
        ],
        axis=0,
    )
    blk = tz["block"]
    shifted = jnp.eye(depth, k=-1, dtype=f32)
    ratio_up = jnp.sum(blk * shifted, axis=0) / tz["diag"]
    sup = jnp.sum(blk * shifted.T, axis=0) / tz["diag"]
    ends = jnp.pad(jnp.stack([tz["from_low"][0], tz["from_high"][-1]]), (0, depth - 2))
    tabs = dict(
        cx=jnp.broadcast_to(jnp.pad(cond_x, (0, 1))[None], (SUB, nx)),
        cup=wide(ye[1:]),
        cdn=wide(ye[:-1]),
        cz=ze,
        wz=jnp.stack([blk[-1], blk[0]]),
        ay=ay,
        axh=axh,
        axl=axl,
        xlo=xlo,
        xhi=xhi,
        flo=wide(ty["from_low"]),
        fhi=wide(ty["from_high"]),
        coef=jnp.stack([tz["diag"], ratio_up, sup, ends]),
    )
    u = phase_field
    for step in range(STEPS):
        t, sy, sz = explicit(u, others, halo(u), tabs)
        p, q = carries_paired(sy, ty, "gy")
        zl, zr = carries_direct(sz[0], sz[1], tz, "gz")
        pq = jnp.stack([p, q])
        up = jnp.sum(pq * tabs["wz"][0][None, :, None], axis=1)
        down = jnp.sum(pq * tabs["wz"][1][None, :, None], axis=1)
        cl, cr = carries_direct(up, down, tz, "gz")
        lo, hi = ty["from_low"][:, None], ty["from_high"][:, None]
        zl = zl + lo * cl[0] + hi * cl[1]
        zr = zr + lo * cr[0] + hi * cr[1]
        u = update(t, u, p, q, zl, zr, tabs)
    return u


def solution(mesh):
    placed = (P("gz", "gy", None), P("gz", "gy", None), P(), P(), P(), P(), P(), P())
    return jax.shard_map(
        body, mesh=mesh, in_specs=placed, out_specs=P("gz", "gy", None), check_vma=False
    )
```

```python
import functools

import jax
import jax.numpy as jnp
from jax import lax
from jax.experimental import pallas as pl
from jax.experimental.pallas import tpu as pltpu
from jax.sharding import PartitionSpec as P


STEPS = 2
REACTION = 2.0
LANES = 128
SUB = 8
XB = 256
ZB = 8

DIAG, UP, DOWN, SUM_UP, SUM_DOWN, COND, MISC, CHIPS, LINES = range(9)
TABLE_ROWS = 16
Z_LOW, Z_HIGH, Y_LOW, Y_HIGH, MIX, KEEP, GIVE = 0, 1, 2, 3, 4, 8, 12
FAR = 64

f32 = jnp.float32
bf16 = jnp.bfloat16


def split(a):
    high = a.astype(bf16)
    low = (a - high.astype(f32)).astype(bf16)
    return high, low


def wide_rows(ref, rows, nx):
    return jnp.concatenate([ref[rows]] * (nx // LANES), axis=1)


def full(a):
    return pl.BlockSpec(a.shape, lambda *_: (0,) * len(a.shape))


def smem():
    return pl.BlockSpec(memory_space=pltpu.SMEM)


def call(kernel, out_shape, operands, **kw):
    limit = kw.pop("vmem", 16)
    return pl.pallas_call(
        kernel,
        out_shape=out_shape,
        compiler_params=pltpu.CompilerParams(
            dimension_semantics=("arbitrary",) * len(kw.get("grid", ())),
            vmem_limit_bytes=limit * 2**20,
        ),
        **kw,
    )(*operands)


def shape(*dims, dtype=f32):
    return jax.ShapeDtypeStruct(dims, dtype)


def strip_of(ref, start, count):
    total = ref.shape[0]
    top = pl.multiple_of(lax.rem(start - SUB + total, total), SUB)
    end = pl.multiple_of(lax.rem(start + count, total), SUB)
    rows = jnp.concatenate(
        [
            ref[pl.ds(top, SUB), :],
            ref[pl.ds(pl.multiple_of(start, SUB), count), :],
            ref[pl.ds(end, SUB), :],
        ],
        axis=0,
    )
    return pltpu.roll(rows, lax.rem(total - start, total), 1)


def entry(ref, i, j):
    total = ref.shape[0]
    i = lax.rem(i + total, total)
    j = lax.rem(j + total, total)
    row = ref[pl.ds(i, 1), :]
    lane = lax.broadcasted_iota(jnp.int32, row.shape, 1)
    return jnp.sum(jnp.where(lane == j, row, 0.0), axis=1, keepdims=True)


def over_pivot(ref, i, j):
    return entry(ref, i, j) / entry(ref, j, j)


def tables_kernel(
    ids_ref, ax_ref, lower_ref, lpiv_ref, upper_ref, upiv_ref, ay_ref, az_ref,
    cy_ref, cz_ref,
    axh_ref, axl_ref, xlo_ref, xhi_ref, wide_ref, mat_ref, scal_ref,
    *, rows, depth, ny, nz,
):
    e = pl.program_id(0)
    last = pl.num_programs(0) - 1
    high, low = split(ax_ref[...].T)
    axh_ref[0] = high
    axl_ref[0] = low
    from_low = lower_ref[...].T[LANES - 1 :] / lpiv_ref[SUB - 1 :, LANES - 1 :]
    from_high = upper_ref[...].T[:1] / upiv_ref[:1, :1]
    xlo_ref[...] = jnp.where(e > 0, from_low, 0.0)
    xhi_ref[...] = jnp.where(e < last, from_high, 0.0)

    @pl.when(e == 0)
    def _():
        gy, gz = ids_ref[0], ids_ref[1]
        y0, z0 = gy * rows, gz * depth
        ys = strip_of(ay_ref, y0, rows)
        zs = strip_of(az_ref, z0, depth)
        end = ay_ref.shape[0] - 1
        pad = jnp.zeros((SUB - 2, 1), f32)

        def arranged(column):
            return jnp.concatenate(
                [
                    column[SUB : SUB + rows],
                    column[SUB - 1 : SUB],
                    column[SUB + rows : SUB + rows + 1],
                    pad,
                ],
                axis=0,
            )

        lo = arranged(ys[:, end:] / ys[SUB - 1 : SUB, end:])
        hi = arranged(
            ys[:, rows : rows + 1] / ys[SUB + rows : SUB + rows + 1, rows : rows + 1]
        )
        wide_ref[0] = jnp.broadcast_to(lo, (rows + SUB, LANES))
        wide_ref[1] = jnp.broadcast_to(hi, (rows + SUB, LANES))
        cy = pltpu.roll(cy_ref[...], lax.rem(cy_ref.shape[1] - y0, cy_ref.shape[1]), 1)
        cy = jnp.broadcast_to(cy[:, :LANES], (LANES, LANES)).T
        wide_ref[2] = cy[1 : rows + 1 + SUB]
        wide_ref[3] = cy[: rows + SUB]
        bh, bl = split(ys[SUB : SUB + rows, :rows])
        mat_ref[:rows, :] = jnp.concatenate([bh, bh], axis=1)
        mat_ref[rows:, :] = jnp.concatenate([bl, jnp.zeros_like(bl)], axis=1)

        total = az_ref.shape[0]
        r = lax.broadcasted_iota(jnp.int32, zs.shape, 0)
        c = lax.broadcasted_iota(jnp.int32, zs.shape, 1)
        pick = lambda shift: jnp.sum(
            jnp.where(r == c + (SUB + shift), zs, 0.0), axis=0, keepdims=True
        )
        lane = lax.broadcasted_iota(jnp.int32, (1, total), 1)
        diag = jnp.where(lane < depth, pick(0), 1.0)
        scal_ref[...] = jnp.zeros_like(scal_ref)

        def row(index, value):
            scal_ref[index : index + 1, :] = value[:, :LANES]

        row(DIAG, diag)
        row(UP, pick(1) / diag)
        row(DOWN, pick(-1) / diag)
        row(SUM_UP, zs[SUB + depth - 1 : SUB + depth])
        row(SUM_DOWN, zs[SUB : SUB + 1])
        cz = pltpu.roll(cz_ref[...], lax.rem(cz_ref.shape[1] - z0, cz_ref.shape[1]), 1)
        row(COND, cz)

        lane = lax.broadcasted_iota(jnp.int32, (1, LANES), 1)

        def fill(index, values):
            line = jnp.zeros((1, LANES), f32)
            for at, value in values.items():
                line = jnp.where(lane == at, value, line)
            row(index, line)

        far = total - 1
        core = lax.rem(gy, 2)
        chip = gy // 2
        chips = ny // 2
        yb = chip * (2 * rows)
        one = jnp.ones((1, 1), f32)
        zero = jnp.zeros((1, 1), f32)
        up = over_pivot(ay_ref, yb + 2 * rows - 1, yb + rows - 1)
        down = over_pivot(ay_ref, yb, yb + rows)
        through_up = over_pivot(ay_ref, yb + rows - 1, yb - 1)
        through_down = over_pivot(ay_ref, yb + rows, yb + 2 * rows)
        by_core = lambda a, b: jnp.where(core == 0, a, b)
        fill(
            MISC,
            {
                Z_LOW: zs[SUB : SUB + 1, far:] / zs[SUB - 1 : SUB, far:],
                Z_HIGH: zs[SUB + depth - 1 : SUB + depth, depth : depth + 1]
                / zs[SUB + depth : SUB + depth + 1, depth : depth + 1],
                Y_LOW: ys[SUB - 1 : SUB, :1] / ys[SUB : SUB + 1, :1],
                Y_HIGH: ys[SUB + rows : SUB + rows + 1, rows - 1 : rows]
                / ys[SUB + rows - 1 : SUB + rows, rows - 1 : rows],
                MIX: by_core(up, one),
                MIX + 1: by_core(one, up),
                MIX + 2: by_core(one, down),
                MIX + 3: by_core(down, one),
                KEEP: by_core(one, through_up),
                KEEP + 1: by_core(zero, one),
                KEEP + 2: by_core(through_down, one),
                KEEP + 3: by_core(one, zero),
                GIVE: by_core(through_up, one),
                GIVE + 1: by_core(one, zero),
                GIVE + 2: by_core(one, through_down),
                GIVE + 3: by_core(zero, one),
            },
        )
        values = {}
        for k in range(1, chips):
            src = lax.rem(chip - k + chips, chips)
            below = src < chip
            a = over_pivot(ay_ref, yb - 1, (src + 1) * 2 * rows - 1)
            b = over_pivot(ay_ref, yb + 2 * rows, src * 2 * rows)
            values[k] = jnp.where(below, a, 0.0)
            values[FAR + k] = jnp.where(below, 0.0, b)
        fill(CHIPS, values)
        values = {}
        for k in range(1, nz):
            src = lax.rem(gz - k + nz, nz)
            below = src < gz
            a = over_pivot(az_ref, z0 - 1, (src + 1) * depth - 1)
            b = over_pivot(az_ref, z0 + depth, src * depth)
            values[k] = jnp.where(below, a, 0.0)
            values[FAR + k] = jnp.where(below, 0.0, b)
        fill(LINES, values)


def tables(ids, inverse_x, inverse_y, inverse_z, cond_y, cond_z, rows, depth):
    nx = inverse_x.shape[0]
    blocks = nx // XB
    ny, nz = lax.axis_size("gy"), lax.axis_size("gz")
    q, s = XB // LANES, XB // SUB
    round_up = lambda n: -(-n // LANES) * LANES
    cy = jnp.pad(cond_y, (1, round_up(cond_y.shape[0] + 2 + LANES) - cond_y.shape[0] - 1))[None]
    cz = jnp.pad(cond_z, (1, round_up(cond_z.shape[0] + 2 + LANES) - cond_z.shape[0] - 1))[None]
    column = lambda at: pl.BlockSpec((XB, LANES), lambda e: (e, at(e)))
    low = lambda e: jnp.maximum(q * e - 1, 0)
    top = lambda e: jnp.minimum(q * e + q, q * blocks - 1)
    return call(
        functools.partial(tables_kernel, rows=rows, depth=depth, ny=ny, nz=nz),
        [
            shape(blocks, XB, XB, dtype=bf16),
            shape(blocks, XB, XB, dtype=bf16),
            shape(1, nx),
            shape(1, nx),
            shape(4, rows + SUB, LANES),
            shape(2 * rows, 2 * rows, dtype=bf16),
            shape(TABLE_ROWS, LANES),
        ],
        (ids, inverse_x, inverse_x, inverse_x, inverse_x, inverse_x, inverse_y, inverse_z, cy, cz),
        grid=(blocks,),
        in_specs=[
            smem(),
            pl.BlockSpec((XB, XB), lambda e: (e, e)),
            column(low),
            pl.BlockSpec((SUB, LANES), lambda e: (jnp.maximum(s * e - 1, 0), low(e))),
            column(top),
            pl.BlockSpec(
                (SUB, LANES), lambda e: (jnp.minimum(s * e + s, s * blocks - 1), top(e))
            ),
            full(inverse_y), full(inverse_z), full(cy), full(cz),
        ],
        out_specs=[
            pl.BlockSpec((1, XB, XB), lambda e: (e, 0, 0)),
            pl.BlockSpec((1, XB, XB), lambda e: (e, 0, 0)),
            pl.BlockSpec((1, XB), lambda e: (0, e)),
            pl.BlockSpec((1, XB), lambda e: (0, e)),
            full(shape(4, rows + SUB, LANES)),
            full(shape(2 * rows, 2 * rows)),
            full(shape(TABLE_ROWS, LANES)),
        ],
        name="tables",
    )


def explicit_kernel(
    ids_ref, scal_ref, u_ref, below_ref, above_ref, o_ref, ylo_ref, yhi_ref,
    zlo_ref, zhi_ref, cx_ref, wide_ref, ay_ref, axh_ref, axl_ref, xlo_ref, xhi_ref,
    t_ref, edge_ref, mine_ref, theirs_ref, *rest, nz,
):
    pays = rest[: nz - 1]
    rhs_ref, line_ref, sy_ref, sz_ref, low_ref, high_ref = rest[nz - 1 :]
    step = pl.program_id(0)
    steps = pl.num_programs(0)
    zb, rows, nx = u_ref.shape
    tiles = rows // SUB
    blocks = nx // XB
    sub = lax.broadcasted_iota(jnp.int32, (SUB, nx), 0)

    low_ref[...] = jnp.where(step > 0, below_ref[0], zlo_ref[...])
    high_ref[...] = jnp.where(step < steps - 1, above_ref[0], zhi_ref[...])

    def plane(z, below, above):
        zz = step * zb + z
        c_dn = scal_ref[COND, zz]
        c_up = scal_ref[COND, zz + 1]
        cx = jnp.broadcast_to(cx_ref[...], (SUB, nx))
        before = jnp.broadcast_to(ylo_ref[pl.ds(zz, 1), :], (SUB, nx))
        current = u_ref[z, :SUB, :]
        down_roll = pltpu.roll(current, 1, 0)
        for r in range(tiles):
            own = slice(r * SUB, (r + 1) * SUB)
            if r + 1 < tiles:
                following = u_ref[z, (r + 1) * SUB : (r + 2) * SUB, :]
                up_next = pltpu.roll(following, SUB - 1, 0)
                down_next = pltpu.roll(following, 1, 0)
            else:
                following = down_next = None
                up_next = jnp.broadcast_to(yhi_ref[pl.ds(zz, 1), :], (SUB, nx))
            c = current
            down = jnp.where(sub == 0, before, down_roll)
            up = jnp.where(sub == SUB - 1, up_next, pltpu.roll(c, SUB - 1, 0))
            fx = (pltpu.roll(c, nx - 1, 1) - c) * cx
            total = fx - pltpu.roll(fx, 1, 1)
            cup = wide_rows(wide_ref, (2, own), nx)
            cdn = wide_rows(wide_ref, (3, own), nx)
            total = total + ((up - c) * cup - (c - down) * cdn)
            total = total + ((above(own) - c) * c_up - (c - below(own)) * c_dn)
            o = o_ref[z, own, :]
            total = total + (REACTION * c) * (1.0 - c * c - 2.0 * o)
            rhs_ref[pl.ds(pl.multiple_of(z * rows + r * SUB, SUB), SUB), :] = total
            before = down_roll
            current = following
            down_roll = down_next

    plane(0, lambda own: low_ref[own, :], lambda own: u_ref[1, own, :])

    def inner(z, carry):
        plane(z, lambda own: u_ref[z - 1, own, :], lambda own: u_ref[z + 1, own, :])
        return carry

    lax.fori_loop(1, zb - 1, inner, 0)
    plane(zb - 1, lambda own: u_ref[zb - 2, own, :], lambda own: high_ref[own, :])

    dot = functools.partial(jnp.dot, preferred_element_type=f32)
    for e in range(blocks):
        cols = slice(e * XB, (e + 1) * XB)
        high, low = split(rhs_ref[:, cols])
        line_ref[:, cols] = (
            dot(high, axh_ref[e]) + dot(low, axh_ref[e]) + dot(high, axl_ref[e])
        )
    lows = [None]
    for e in range(blocks - 1):
        at = slice((e + 1) * XB - 1, (e + 1) * XB)
        end = line_ref[:, at]
        if lows[e] is not None:
            end = end + lows[e] * xlo_ref[:, at]
        lows.append(end)
    highs = [None] * blocks
    for e in reversed(range(1, blocks)):
        at = slice(e * XB, e * XB + 1)
        end = line_ref[:, at]
        if highs[e] is not None:
            end = end + highs[e] * xhi_ref[:, at]
        highs[e - 1] = end
    for e in range(blocks):
        cols = slice(e * XB, (e + 1) * XB)
        value = line_ref[:, cols]
        if lows[e] is not None:
            value = value + lows[e] * xlo_ref[:, cols]
        if highs[e] is not None:
            value = value + highs[e] * xhi_ref[:, cols]
        line_ref[:, cols] = value

    @pl.when(step == 0)
    def _():
        sz_ref[...] = jnp.zeros_like(sz_ref)

    y_low = scal_ref[MISC, Y_LOW]
    y_high = scal_ref[MISC, Y_HIGH]

    def solve(z, carry):
        zz = step * zb + z
        base = pl.multiple_of(z * rows, rows)
        high, low = split(line_ref[pl.ds(base, rows), :])
        both = jnp.concatenate([high, low], axis=0)
        result = dot(ay_ref[...], both)
        value = result[:rows] + result[rows:]
        t_ref[z] = value
        first, final = value[:1], value[rows - 1 :]
        sy_ref[0, pl.ds(z, 1), :] = final
        sy_ref[1, pl.ds(z, 1), :] = first
        edge_ref[z, 0:1, :] = y_low * first
        edge_ref[z, 1:2, :] = y_high * final
        sz_ref[0] = sz_ref[0] + scal_ref[SUM_UP, zz] * value
        sz_ref[1] = sz_ref[1] + scal_ref[SUM_DOWN, zz] * value
        return carry

    lax.fori_loop(0, zb, solve, 0)

    half = mine_ref.shape[1]
    part = (step * zb) // half
    at = pl.ds(pl.multiple_of(step * zb - part * half, SUB), zb)
    core = lax.rem(ids_ref[0], 2)

    @pl.when(part == core)
    def _():
        mine_ref[:, at, :] = sy_ref[...]

    @pl.when(part != core)
    def _():
        theirs_ref[:, at, :] = sy_ref[...]

    @pl.when(step == steps - 1)
    def _():
        for k in range(1, nz):
            higher = ids_ref[1] + k < nz
            pays[k - 1][...] = jnp.where(higher, sz_ref[0], sz_ref[1])


def explicit(ids, scal, u, o, halos, tabs, cx):
    depth, rows, nx = u.shape
    axh, axl, xlo, xhi, wide, mat = tabs
    nz = lax.axis_size("gz")
    zb = ZB
    steps = depth // zb
    half = depth // 2
    field = pl.BlockSpec((zb, rows, nx), lambda s: (s, 0, 0))
    below = pl.BlockSpec((1, rows, nx), lambda s: (jnp.maximum(s * zb - 1, 0), 0, 0))
    above = pl.BlockSpec(
        (1, rows, nx), lambda s: (jnp.minimum(s * zb + zb, depth - 1), 0, 0)
    )
    rest = (*halos, cx, wide, mat, axh, axl, xlo, xhi)
    outs = [
        shape(depth, rows, nx),
        shape(depth, SUB, nx),
        shape(2, half, nx),
        shape(2, half, nx),
    ] + [shape(rows, nx)] * (nz - 1)
    return call(
        functools.partial(explicit_kernel, nz=nz),
        outs,
        (ids, scal, u, u, u, o, *rest),
        grid=(steps,),
        in_specs=[smem(), smem(), field, below, above, field, *map(full, rest)],
        out_specs=[field, pl.BlockSpec((zb, SUB, nx), lambda s: (s, 0, 0))]
        + [full(a) for a in outs[2:]],
        scratch_shapes=[
            pltpu.VMEM((zb * rows, nx), f32),
            pltpu.VMEM((zb * rows, nx), f32),
            pltpu.VMEM((2, zb, nx), f32),
            pltpu.VMEM((2, rows, nx), f32),
            pltpu.VMEM((rows, nx), f32),
            pltpu.VMEM((rows, nx), f32),
        ],
        vmem=48,
        name="explicit",
    )


def chip_kernel(ids_ref, scal_ref, mine_ref, other_ref, *pays):
    mix = lambda i: scal_ref[MISC, MIX + i]
    up = mix(0) * mine_ref[0] + mix(1) * other_ref[0]
    down = mix(2) * mine_ref[1] + mix(3) * other_ref[1]
    chip = ids_ref[0] // 2
    for k, pay in enumerate(pays, 1):
        pay[...] = jnp.where(chip + k < len(pays) + 1, up, down)


def share_kernel(scal_ref, mine_ref, other_ref, *rest):
    *gots, keep_ref, give_ref = rest
    low = jnp.zeros_like(gots[0])
    high = jnp.zeros_like(gots[0])
    for k, got in enumerate(gots, 1):
        low = low + scal_ref[CHIPS, k] * got[...]
        high = high + scal_ref[CHIPS, FAR + k] * got[...]
    keep = lambda i: scal_ref[MISC, KEEP + i]
    give = lambda i: scal_ref[MISC, GIVE + i]
    keep_ref[0] = keep(0) * low + keep(1) * other_ref[0]
    keep_ref[1] = keep(2) * high + keep(3) * other_ref[1]
    give_ref[0] = give(0) * low + give(1) * mine_ref[0]
    give_ref[1] = give(2) * high + give(3) * mine_ref[1]


def corner_kernel(ids_ref, scal_ref, keep_ref, back_ref, *pays):
    half = keep_ref.shape[1]
    core = lax.rem(ids_ref[0], 2)
    near, far = core * half, (1 - core) * half
    up = jnp.zeros((2, keep_ref.shape[2]), f32)
    down = jnp.zeros_like(up)
    for z in range(half):
        for ref, base in ((keep_ref, near), (back_ref, far)):
            row = ref[:, z, :]
            up = up + scal_ref[SUM_UP, base + z] * row
            down = down + scal_ref[SUM_DOWN, base + z] * row
    for k, pay in enumerate(pays, 1):
        pay[...] = jnp.where(ids_ref[1] + k < len(pays) + 1, up, down)


def cyclic(size, k, stride=1):
    groups = size // stride
    return [
        (c * stride + r, ((c + k) % groups) * stride + r)
        for c in range(groups)
        for r in range(stride)
    ]


def update_kernel(
    ids_ref, scal_ref, t_ref, u_ref, edge_ref, keep_ref, back_ref, wide_ref,
    ylo_ref, yhi_ref, zlo_ref, zhi_ref, *rest, nz, final,
):
    gots, corners, rest = rest[: nz - 1], rest[nz - 1 : 2 * nz - 2], rest[2 * nz - 2 :]
    if final:
        out_ref, e_ref, pq_ref = rest
    else:
        out_ref, nylo_ref, nyhi_ref, nzlo_ref, nzhi_ref, e_ref, pq_ref, s_ref = rest
    r = pl.program_id(0)
    depth, _, nx = t_ref.shape
    half = keep_ref.shape[1]
    tiles = wide_ref.shape[1] // SUB - 1
    scal = lambda i, j: scal_ref[i, j]

    @pl.when(r == 0)
    def _():
        core = lax.rem(ids_ref[0], 2)
        near = pl.multiple_of(core * half, SUB)
        far = pl.multiple_of((1 - core) * half, SUB)
        pq_ref[:, pl.ds(near, half), :] = keep_ref[...]
        pq_ref[:, pl.ds(far, half), :] = back_ref[...]

    own = pl.ds(pl.multiple_of(r * SUB, SUB), SUB)
    lo = wide_rows(wide_ref, (0, own), nx)
    hi = wide_rows(wide_ref, (1, own), nx)

    def solve(carry_rows, get_t, put_first, put_second):
        low = jnp.zeros((SUB, nx), f32)
        high = jnp.zeros((SUB, nx), f32)
        for k in range(1, nz):
            value = carry_rows(gots[k - 1])
            value = value + lo * corners[k - 1][0:1, :] + hi * corners[k - 1][1:2, :]
            low = low + scal(LINES, k) * value
            high = high + scal(LINES, FAR + k) * value

        def forward(z, carry):
            v = get_t(z) + lo * pq_ref[0, pl.ds(z, 1), :] + hi * pq_ref[1, pl.ds(z, 1), :]
            e = scal(DIAG, z) * v
            e_ref[z] = e
            s = carry + e
            put_first(z, s)
            return scal(UP, z) * s

        above = lax.fori_loop(0, depth, forward, scal(MISC, Z_LOW) * low, unroll=4)

        def backward(k, carry):
            z = depth - 1 - k
            put_second(z, carry)
            return scal(DOWN, z) * (carry + e_ref[z])

        below = lax.fori_loop(0, depth, backward, scal(MISC, Z_HIGH) * high, unroll=4)
        return low + below, high + above

    def first(z, s):
        out_ref[z] = u_ref[z] + s

    def second(z, b):
        out_ref[z] = out_ref[z] + b

    @pl.when(r < tiles)
    def _():
        below, above = solve(lambda got: got[own, :], lambda z: t_ref[z], first, second)
        if not final:
            nzlo_ref[...] = zlo_ref[...] + below
            nzhi_ref[...] = zhi_ref[...] + above

    if not final:
        y_low = scal(MISC, Y_LOW)
        y_high = scal(MISC, Y_HIGH)
        pad = jnp.zeros((SUB - 2, nx), f32)

        def ends(got):
            rows = got.shape[0]
            return jnp.concatenate(
                [y_low * got[0:1, :], y_high * got[rows - 1 : rows, :], pad], axis=0
            )

        def keep_sum(z, s):
            s_ref[z] = s

        def put(z, b):
            value = s_ref[z] + b
            nylo_ref[pl.ds(z, 1), :] = ylo_ref[pl.ds(z, 1), :] + value[0:1]
            nyhi_ref[pl.ds(z, 1), :] = yhi_ref[pl.ds(z, 1), :] + value[1:2]

        @pl.when(r == tiles)
        def _():
            solve(ends, lambda z: edge_ref[z], keep_sum, put)


def update(ids, scal, t, u, edge, keep, back, wide, halos, gots, corners, final):
    depth, rows, nx = u.shape
    nz = lax.axis_size("gz")
    tiles = rows // SUB
    ylo, yhi, zlo, zhi = halos
    clamp = lambda r: jnp.minimum(r, tiles - 1)
    field = pl.BlockSpec((depth, SUB, nx), lambda r: (0, clamp(r), 0))
    tile = pl.BlockSpec((SUB, nx), lambda r: (clamp(r), 0))
    outs = [shape(depth, rows, nx)]
    out_specs = [field]
    scratch = [pltpu.VMEM((depth, SUB, nx), f32), pltpu.VMEM((2, depth, nx), f32)]
    if not final:
        outs += [shape(depth, nx)] * 2 + [shape(rows, nx)] * 2
        out_specs += [full(ylo), full(yhi), tile, tile]
        scratch += [pltpu.VMEM((depth, SUB, nx), f32)]
    return call(
        functools.partial(update_kernel, nz=nz, final=final),
        outs,
        (ids, scal, t, u, edge, keep, back, wide, ylo, yhi, zlo, zhi, *gots, *corners),
        grid=(tiles if final else tiles + 1,),
        in_specs=[
            smem(), smem(), field, field, full(edge), full(keep), full(back), full(wide),
            full(ylo), full(yhi), tile, tile,
            *map(full, gots), *map(full, corners),
        ],
        out_specs=out_specs,
        scratch_shapes=scratch,
        vmem=32,
        name="update",
    )


def halo(u):
    ny, nz = lax.axis_size("gy"), lax.axis_size("gz")
    up = lambda n: [(i, i + 1) for i in range(n - 1)]
    down = lambda n: [(i + 1, i) for i in range(n - 1)]
    ylo = lax.ppermute(u[:, -1, :], "gy", up(ny))
    yhi = lax.ppermute(u[:, 0, :], "gy", down(ny))
    zlo = lax.ppermute(u[-1], "gz", up(nz))
    zhi = lax.ppermute(u[0], "gz", down(nz))
    return ylo, yhi, zlo, zhi


def body(phase_field, others, cond_x, cond_y, cond_z, inverse_x, inverse_y, inverse_z):
    depth, rows, nx = phase_field.shape
    ny, nz = lax.axis_size("gy"), lax.axis_size("gz")
    half = depth // 2
    ids = jnp.stack([lax.axis_index("gy"), lax.axis_index("gz")])
    halos = halo(phase_field)
    *tabs, scal = tables(
        ids, inverse_x, inverse_y, inverse_z, cond_y, cond_z, rows, depth
    )
    wide = tabs[4]
    cx = jnp.pad(cond_x, (0, 1))[None]
    swap = [(i, i ^ 1) for i in range(ny)]
    u = phase_field
    for step in range(STEPS):
        final = step == STEPS - 1
        t, edge, mine, theirs, *pays = explicit(ids, scal, u, others, halos, tabs, cx)
        gots = []
        for k in range(1, nz):
            gots.append(lax.ppermute(pays[k - 1], "gz", cyclic(nz, k)))
        other = lax.ppermute(theirs, "gy", swap)
        pays = call(
            chip_kernel,
            [shape(half, nx)] * (ny // 2 - 1),
            (ids, scal, mine, other),
            in_specs=[smem(), smem(), full(mine), full(other)],
            name="chip",
        )
        moved = [
            lax.ppermute(pays[k - 1], "gy", cyclic(ny, k, 2))
            for k in range(1, ny // 2)
        ]
        keep, give = call(
            share_kernel,
            [shape(2, half, nx)] * 2,
            (scal, mine, other, *moved),
            in_specs=[smem(), full(mine), full(other), *map(full, moved)],
            name="share",
        )
        back = lax.ppermute(give, "gy", swap)
        pays = call(
            corner_kernel,
            [shape(2, nx)] * (nz - 1),
            (ids, scal, keep, back),
            in_specs=[smem(), smem(), full(keep), full(back)],
            name="corner",
        )
        corners = [lax.ppermute(pays[k - 1], "gz", cyclic(nz, k)) for k in range(1, nz)]
        out = update(
            ids, scal, t, u, edge, keep, back, wide, halos, gots, corners, final
        )
        u, halos = out[0], out[1:]
    return u


def solution(mesh):
    placed = (P("gz", "gy", None), P("gz", "gy", None), P(), P(), P(), P(), P(), P())
    return jax.shard_map(
        body, mesh=mesh, in_specs=placed, out_specs=P("gz", "gy", None), check_vma=False
    )
```

```python
import functools

import jax
import jax.numpy as jnp
from jax import lax
from jax.experimental import pallas as pl
from jax.experimental.pallas import tpu as pltpu
from jax.sharding import PartitionSpec as P


STEPS = 2
REACTION = 2.0
LANES = 128
SUB = 8
XB = 256
ZB = 8
VL1 = 30
VL2 = 20

DIAG, UP, DOWN, SUM_UP, SUM_DOWN, COND, MISC, CHIPS, LINES = range(9)
TABLE_ROWS = 16
Z_LOW, Z_HIGH, Y_LOW, Y_HIGH, MIX, KEEP, GIVE = 0, 1, 2, 3, 4, 8, 12
LARGE = 2**20
FAR = 64

f32 = jnp.float32
bf16 = jnp.bfloat16


def split(a):
    high = a.astype(bf16)
    low = (a - high.astype(f32)).astype(bf16)
    return high, low


def wide_rows(ref, rows, nx):
    return jnp.concatenate([ref[rows]] * (nx // LANES), axis=1)


VMEM_WHOLE = pl.BlockSpec(memory_space=pltpu.VMEM)


def full(a):
    return pl.BlockSpec(a.shape, lambda *_: (0,) * len(a.shape))


def smem():
    return pl.BlockSpec(memory_space=pltpu.SMEM)


def call(kernel, out_shape, operands, **kw):
    limit = kw.pop("vmem", 16)
    large = kw.pop("large", LARGE)
    resident = kw.pop("resident", ())
    operands = [
        pltpu.with_memory_space_constraint(a, pltpu.HBM)
        if a.size >= large and s is not VMEM_WHOLE
        else a
        for a, s in zip(operands, kw["in_specs"])
    ]
    out_shape = [
        pltpu.VMEM(a.shape, a.dtype)
        if i in resident
        else pltpu.HBM(a.shape, a.dtype)
        if a.size >= large
        else a
        for i, a in enumerate(out_shape)
    ]
    return pl.pallas_call(
        kernel,
        out_shape=out_shape,
        compiler_params=pltpu.CompilerParams(
            dimension_semantics=("arbitrary",) * len(kw.get("grid", ())),
            vmem_limit_bytes=limit * 2**20,
        ),
        **kw,
    )(*operands)


def shape(*dims, dtype=f32):
    return jax.ShapeDtypeStruct(dims, dtype)


def strip_of(ref, start, count):
    total = ref.shape[0]
    top = pl.multiple_of(lax.rem(start - SUB + total, total), SUB)
    end = pl.multiple_of(lax.rem(start + count, total), SUB)
    rows = jnp.concatenate(
        [
            ref[pl.ds(top, SUB), :],
            ref[pl.ds(pl.multiple_of(start, SUB), count), :],
            ref[pl.ds(end, SUB), :],
        ],
        axis=0,
    )
    return pltpu.roll(rows, lax.rem(total - start, total), 1)


def entry(ref, i, j):
    total = ref.shape[0]
    i = lax.rem(i + total, total)
    j = lax.rem(j + total, total)
    row = ref[pl.ds(i, 1), :]
    lane = lax.broadcasted_iota(jnp.int32, row.shape, 1)
    return jnp.sum(jnp.where(lane == j, row, 0.0), axis=1, keepdims=True)


def over_pivot(ref, i, j):
    return entry(ref, i, j) / entry(ref, j, j)


def tables_kernel(
    ids_ref, ax_ref, lower_ref, lpiv_ref, upper_ref, upiv_ref, ay_ref, az_ref,
    cy_ref, cz_ref,
    axh_ref, axl_ref, xlo_ref, xhi_ref, wide_ref, mat_ref, scal_ref,
    *, rows, depth, ny, nz,
):
    e = pl.program_id(0)
    last = pl.num_programs(0) - 1
    high, low = split(ax_ref[...].T)
    axh_ref[0] = high
    axl_ref[0] = low
    from_low = lower_ref[...].T[LANES - 1 :] / lpiv_ref[SUB - 1 :, LANES - 1 :]
    from_high = upper_ref[...].T[:1] / upiv_ref[:1, :1]
    xlo_ref[...] = jnp.where(e > 0, from_low, 0.0)
    xhi_ref[...] = jnp.where(e < last, from_high, 0.0)

    @pl.when(e == 0)
    def _():
        gy, gz = ids_ref[0], ids_ref[1]
        y0, z0 = gy * rows, gz * depth
        ys = strip_of(ay_ref, y0, rows)
        zs = strip_of(az_ref, z0, depth)
        end = ay_ref.shape[0] - 1
        pad = jnp.zeros((SUB - 2, 1), f32)

        def arranged(column):
            return jnp.concatenate(
                [
                    column[SUB : SUB + rows],
                    column[SUB - 1 : SUB],
                    column[SUB + rows : SUB + rows + 1],
                    pad,
                ],
                axis=0,
            )

        lo = arranged(ys[:, end:] / ys[SUB - 1 : SUB, end:])
        hi = arranged(
            ys[:, rows : rows + 1] / ys[SUB + rows : SUB + rows + 1, rows : rows + 1]
        )
        wide_ref[0] = jnp.broadcast_to(lo, (rows + SUB, LANES))
        wide_ref[1] = jnp.broadcast_to(hi, (rows + SUB, LANES))
        cy = pltpu.roll(cy_ref[...], lax.rem(cy_ref.shape[1] - y0, cy_ref.shape[1]), 1)
        cy = jnp.broadcast_to(cy[:, :LANES], (LANES, LANES)).T
        wide_ref[2] = cy[1 : rows + 1 + SUB]
        wide_ref[3] = cy[: rows + SUB]
        bh, bl = split(ys[SUB : SUB + rows, :rows])
        mat_ref[:rows, :] = jnp.concatenate([bh, bh], axis=1)
        mat_ref[rows:, :] = jnp.concatenate([bl, jnp.zeros_like(bl)], axis=1)

        total = az_ref.shape[0]
        r = lax.broadcasted_iota(jnp.int32, zs.shape, 0)
        c = lax.broadcasted_iota(jnp.int32, zs.shape, 1)
        pick = lambda shift: jnp.sum(
            jnp.where(r == c + (SUB + shift), zs, 0.0), axis=0, keepdims=True
        )
        lane = lax.broadcasted_iota(jnp.int32, (1, total), 1)
        diag = jnp.where(lane < depth, pick(0), 1.0)
        scal_ref[...] = jnp.zeros_like(scal_ref)

        def row(index, value):
            scal_ref[index : index + 1, :] = value[:, :LANES]

        row(DIAG, diag)
        row(UP, pick(1) / diag)
        row(DOWN, pick(-1) / diag)
        row(SUM_UP, zs[SUB + depth - 1 : SUB + depth])
        row(SUM_DOWN, zs[SUB : SUB + 1])
        cz = pltpu.roll(cz_ref[...], lax.rem(cz_ref.shape[1] - z0, cz_ref.shape[1]), 1)
        row(COND, cz)

        lane = lax.broadcasted_iota(jnp.int32, (1, LANES), 1)

        def fill(index, values):
            line = jnp.zeros((1, LANES), f32)
            for at, value in values.items():
                line = jnp.where(lane == at, value, line)
            row(index, line)

        far = total - 1
        core = lax.rem(gy, 2)
        chip = gy // 2
        chips = ny // 2
        yb = chip * (2 * rows)
        one = jnp.ones((1, 1), f32)
        zero = jnp.zeros((1, 1), f32)
        up = over_pivot(ay_ref, yb + 2 * rows - 1, yb + rows - 1)
        down = over_pivot(ay_ref, yb, yb + rows)
        through_up = over_pivot(ay_ref, yb + rows - 1, yb - 1)
        through_down = over_pivot(ay_ref, yb + rows, yb + 2 * rows)
        by_core = lambda a, b: jnp.where(core == 0, a, b)
        fill(
            MISC,
            {
                Z_LOW: zs[SUB : SUB + 1, far:] / zs[SUB - 1 : SUB, far:],
                Z_HIGH: zs[SUB + depth - 1 : SUB + depth, depth : depth + 1]
                / zs[SUB + depth : SUB + depth + 1, depth : depth + 1],
                Y_LOW: ys[SUB - 1 : SUB, :1] / ys[SUB : SUB + 1, :1],
                Y_HIGH: ys[SUB + rows : SUB + rows + 1, rows - 1 : rows]
                / ys[SUB + rows - 1 : SUB + rows, rows - 1 : rows],
                MIX: by_core(up, one),
                MIX + 1: by_core(one, up),
                MIX + 2: by_core(one, down),
                MIX + 3: by_core(down, one),
                KEEP: by_core(one, through_up),
                KEEP + 1: by_core(zero, one),
                KEEP + 2: by_core(through_down, one),
                KEEP + 3: by_core(one, zero),
                GIVE: by_core(through_up, one),
                GIVE + 1: by_core(one, zero),
                GIVE + 2: by_core(one, through_down),
                GIVE + 3: by_core(zero, one),
            },
        )
        values = {}
        for k in range(1, chips):
            src = lax.rem(chip - k + chips, chips)
            below = src < chip
            a = over_pivot(ay_ref, yb - 1, (src + 1) * 2 * rows - 1)
            b = over_pivot(ay_ref, yb + 2 * rows, src * 2 * rows)
            values[k] = jnp.where(below, a, 0.0)
            values[FAR + k] = jnp.where(below, 0.0, b)
        fill(CHIPS, values)
        values = {}
        for k in range(1, nz):
            src = lax.rem(gz - k + nz, nz)
            below = src < gz
            a = over_pivot(az_ref, z0 - 1, (src + 1) * depth - 1)
            b = over_pivot(az_ref, z0 + depth, src * depth)
            values[k] = jnp.where(below, a, 0.0)
            values[FAR + k] = jnp.where(below, 0.0, b)
        fill(LINES, values)


def tables(ids, inverse_x, inverse_y, inverse_z, cond_y, cond_z, rows, depth):
    nx = inverse_x.shape[0]
    blocks = nx // XB
    ny, nz = lax.axis_size("gy"), lax.axis_size("gz")
    q, s = XB // LANES, XB // SUB
    round_up = lambda n: -(-n // LANES) * LANES
    cy = jnp.pad(cond_y, (1, round_up(cond_y.shape[0] + 2 + LANES) - cond_y.shape[0] - 1))[None]
    cz = jnp.pad(cond_z, (1, round_up(cond_z.shape[0] + 2 + LANES) - cond_z.shape[0] - 1))[None]
    column = lambda at: pl.BlockSpec((XB, LANES), lambda e: (e, at(e)))
    low = lambda e: jnp.maximum(q * e - 1, 0)
    top = lambda e: jnp.minimum(q * e + q, q * blocks - 1)
    return call(
        functools.partial(tables_kernel, rows=rows, depth=depth, ny=ny, nz=nz),
        [
            shape(blocks, XB, XB, dtype=bf16),
            shape(blocks, XB, XB, dtype=bf16),
            shape(1, nx),
            shape(1, nx),
            shape(4, rows + SUB, LANES),
            shape(2 * rows, 2 * rows, dtype=bf16),
            shape(TABLE_ROWS, LANES),
        ],
        (ids, inverse_x, inverse_x, inverse_x, inverse_x, inverse_x, inverse_y, inverse_z, cy, cz),
        grid=(blocks,),
        in_specs=[
            smem(),
            pl.BlockSpec((XB, XB), lambda e: (e, e)),
            column(low),
            pl.BlockSpec((SUB, LANES), lambda e: (jnp.maximum(s * e - 1, 0), low(e))),
            column(top),
            pl.BlockSpec(
                (SUB, LANES), lambda e: (jnp.minimum(s * e + s, s * blocks - 1), top(e))
            ),
            full(inverse_y), full(inverse_z), full(cy), full(cz),
        ],
        out_specs=[
            pl.BlockSpec((1, XB, XB), lambda e: (e, 0, 0)),
            pl.BlockSpec((1, XB, XB), lambda e: (e, 0, 0)),
            pl.BlockSpec((1, XB), lambda e: (0, e)),
            pl.BlockSpec((1, XB), lambda e: (0, e)),
            full(shape(4, rows + SUB, LANES)),
            full(shape(2 * rows, 2 * rows)),
            full(shape(TABLE_ROWS, LANES)),
        ],
        large=2**14,
        name="tables",
    )


def explicit_kernel(
    ids_ref, scal_ref, *rest, nz, resident,
):
    if resident:
        u_ref, *rest = rest
    else:
        u_ref, below_ref, above_ref, *rest = rest
    o_ref, ylo_ref, yhi_ref, zlo_ref, zhi_ref, cx_ref, wide_ref, *rest = rest
    ay_ref, axh_ref, axl_ref, xlo_ref, xhi_ref, *rest = rest
    t_ref, edge_ref, mine_ref, theirs_ref, *rest = rest
    pays = rest[: nz - 1]
    rhs_ref, line_ref, sy_ref, sz_ref, low_ref, high_ref = rest[nz - 1 :]
    step = pl.program_id(0)
    steps = pl.num_programs(0)
    zb, rows, nx = o_ref.shape
    tiles = rows // SUB
    blocks = nx // XB
    base_z = step * zb if resident else 0
    sub = lax.broadcasted_iota(jnp.int32, (SUB, nx), 0)

    if resident:
        under = u_ref[jnp.maximum(base_z - 1, 0)]
        over = u_ref[jnp.minimum(base_z + zb, steps * zb - 1)]
    else:
        under, over = below_ref[0], above_ref[0]
    low_ref[...] = jnp.where(step > 0, under, zlo_ref[...])
    high_ref[...] = jnp.where(step < steps - 1, over, zhi_ref[...])

    def plane(z, below, above):
        zz = step * zb + z
        c_dn = scal_ref[COND, zz]
        c_up = scal_ref[COND, zz + 1]
        cx = jnp.broadcast_to(cx_ref[...], (SUB, nx))
        before = jnp.broadcast_to(ylo_ref[pl.ds(zz, 1), :], (SUB, nx))
        current = u_ref[base_z + z, :SUB, :]
        down_roll = pltpu.roll(current, 1, 0)
        for r in range(tiles):
            own = slice(r * SUB, (r + 1) * SUB)
            if r + 1 < tiles:
                following = u_ref[base_z + z, (r + 1) * SUB : (r + 2) * SUB, :]
                up_next = pltpu.roll(following, SUB - 1, 0)
                down_next = pltpu.roll(following, 1, 0)
            else:
                following = down_next = None
                up_next = jnp.broadcast_to(yhi_ref[pl.ds(zz, 1), :], (SUB, nx))
            c = current
            down = jnp.where(sub == 0, before, down_roll)
            up = jnp.where(sub == SUB - 1, up_next, pltpu.roll(c, SUB - 1, 0))
            fx = (pltpu.roll(c, nx - 1, 1) - c) * cx
            total = fx - pltpu.roll(fx, 1, 1)
            cup = wide_rows(wide_ref, (2, own), nx)
            cdn = wide_rows(wide_ref, (3, own), nx)
            total = total + ((up - c) * cup - (c - down) * cdn)
            total = total + ((above(own) - c) * c_up - (c - below(own)) * c_dn)
            o = o_ref[z, own, :]
            total = total + (REACTION * c) * (1.0 - c * c - 2.0 * o)
            rhs_ref[pl.ds(pl.multiple_of(z * rows + r * SUB, SUB), SUB), :] = total
            before = down_roll
            current = following
            down_roll = down_next

    plane(0, lambda own: low_ref[own, :], lambda own: u_ref[base_z + 1, own, :])

    def inner(z, carry):
        plane(
            z,
            lambda own: u_ref[base_z + z - 1, own, :],
            lambda own: u_ref[base_z + z + 1, own, :],
        )
        return carry

    lax.fori_loop(1, zb - 1, inner, 0)
    plane(zb - 1, lambda own: u_ref[base_z + zb - 2, own, :], lambda own: high_ref[own, :])

    dot = functools.partial(jnp.dot, preferred_element_type=f32)
    for e in range(blocks):
        cols = slice(e * XB, (e + 1) * XB)
        high, low = split(rhs_ref[:, cols])
        line_ref[:, cols] = (
            dot(high, axh_ref[e]) + dot(low, axh_ref[e]) + dot(high, axl_ref[e])
        )
    lows = [None]
    for e in range(blocks - 1):
        at = slice((e + 1) * XB - 1, (e + 1) * XB)
        end = line_ref[:, at]
        if lows[e] is not None:
            end = end + lows[e] * xlo_ref[:, at]
        lows.append(end)
    highs = [None] * blocks
    for e in reversed(range(1, blocks)):
        at = slice(e * XB, e * XB + 1)
        end = line_ref[:, at]
        if highs[e] is not None:
            end = end + highs[e] * xhi_ref[:, at]
        highs[e - 1] = end
    for e in range(blocks):
        cols = slice(e * XB, (e + 1) * XB)
        value = line_ref[:, cols]
        if lows[e] is not None:
            value = value + lows[e] * xlo_ref[:, cols]
        if highs[e] is not None:
            value = value + highs[e] * xhi_ref[:, cols]
        line_ref[:, cols] = value

    @pl.when(step == 0)
    def _():
        sz_ref[...] = jnp.zeros_like(sz_ref)

    y_low = scal_ref[MISC, Y_LOW]
    y_high = scal_ref[MISC, Y_HIGH]

    def solve(z, carry):
        zz = step * zb + z
        base = pl.multiple_of(z * rows, rows)
        high, low = split(line_ref[pl.ds(base, rows), :])
        both = jnp.concatenate([high, low], axis=0)
        result = dot(ay_ref[...], both)
        value = result[:rows] + result[rows:]
        t_ref[zz] = value
        first, final = value[:1], value[rows - 1 :]
        sy_ref[0, pl.ds(z, 1), :] = final
        sy_ref[1, pl.ds(z, 1), :] = first
        edge_ref[z, 0:1, :] = y_low * first
        edge_ref[z, 1:2, :] = y_high * final
        sz_ref[0] = sz_ref[0] + scal_ref[SUM_UP, zz] * value
        sz_ref[1] = sz_ref[1] + scal_ref[SUM_DOWN, zz] * value
        return carry

    lax.fori_loop(0, zb, solve, 0, unroll=True)

    half = mine_ref.shape[1]
    part = (step * zb) // half
    at = pl.ds(pl.multiple_of(step * zb - part * half, SUB), zb)
    core = lax.rem(ids_ref[0], 2)

    @pl.when(part == core)
    def _():
        mine_ref[:, at, :] = sy_ref[...]

    @pl.when(part != core)
    def _():
        theirs_ref[:, at, :] = sy_ref[...]

    @pl.when(step == steps - 1)
    def _():
        for k in range(1, nz):
            higher = ids_ref[1] + k < nz
            pays[k - 1][...] = jnp.where(higher, sz_ref[0], sz_ref[1])


def explicit(ids, scal, u, o, halos, tabs, cx, resident):
    depth, rows, nx = u.shape
    axh, axl, xlo, xhi, wide, mat = tabs
    nz = lax.axis_size("gz")
    zb = ZB
    steps = depth // zb
    half = depth // 2
    field = pl.BlockSpec((zb, rows, nx), lambda s: (s, 0, 0))
    below = pl.BlockSpec((1, rows, nx), lambda s: (jnp.maximum(s * zb - 1, 0), 0, 0))
    above = pl.BlockSpec(
        (1, rows, nx), lambda s: (jnp.minimum(s * zb + zb, depth - 1), 0, 0)
    )
    rest = (*halos, cx, wide, mat, axh, axl, xlo, xhi)
    outs = [
        shape(depth, rows, nx),
        shape(depth, SUB, nx),
        shape(2, half, nx),
        shape(2, half, nx),
    ] + [shape(rows, nx)] * (nz - 1)
    return call(
        functools.partial(explicit_kernel, nz=nz, resident=resident),
        outs,
        (ids, scal, *([u] if resident else [u, u, u]), o, *rest),
        grid=(steps,),
        in_specs=[smem(), smem()]
        + ([VMEM_WHOLE] if resident else [field, below, above])
        + [field, *map(full, rest)],
        resident=(0,),
        out_specs=[VMEM_WHOLE, pl.BlockSpec((zb, SUB, nx), lambda s: (s, 0, 0))]
        + [full(a) for a in outs[2:]],
        scratch_shapes=[
            pltpu.VMEM((zb * rows, nx), f32),
            pltpu.VMEM((zb * rows, nx), f32),
            pltpu.VMEM((2, zb, nx), f32),
            pltpu.VMEM((2, rows, nx), f32),
            pltpu.VMEM((rows, nx), f32),
            pltpu.VMEM((rows, nx), f32),
        ],
        vmem=VL1,
        name="explicit",
    )


def chip_kernel(ids_ref, scal_ref, mine_ref, other_ref, *pays):
    mix = lambda i: scal_ref[MISC, MIX + i]
    up = mix(0) * mine_ref[0] + mix(1) * other_ref[0]
    down = mix(2) * mine_ref[1] + mix(3) * other_ref[1]
    chip = ids_ref[0] // 2
    for k, pay in enumerate(pays, 1):
        pay[...] = jnp.where(chip + k < len(pays) + 1, up, down)


def share_kernel(scal_ref, mine_ref, other_ref, *rest):
    *gots, keep_ref, give_ref = rest
    low = jnp.zeros_like(gots[0])
    high = jnp.zeros_like(gots[0])
    for k, got in enumerate(gots, 1):
        low = low + scal_ref[CHIPS, k] * got[...]
        high = high + scal_ref[CHIPS, FAR + k] * got[...]
    keep = lambda i: scal_ref[MISC, KEEP + i]
    give = lambda i: scal_ref[MISC, GIVE + i]
    keep_ref[0] = keep(0) * low + keep(1) * other_ref[0]
    keep_ref[1] = keep(2) * high + keep(3) * other_ref[1]
    give_ref[0] = give(0) * low + give(1) * mine_ref[0]
    give_ref[1] = give(2) * high + give(3) * mine_ref[1]


def corner_kernel(ids_ref, scal_ref, keep_ref, back_ref, *pays):
    half = keep_ref.shape[1]
    core = lax.rem(ids_ref[0], 2)
    near, far = core * half, (1 - core) * half
    up = jnp.zeros((2, keep_ref.shape[2]), f32)
    down = jnp.zeros_like(up)
    for z in range(half):
        for ref, base in ((keep_ref, near), (back_ref, far)):
            row = ref[:, z, :]
            up = up + scal_ref[SUM_UP, base + z] * row
            down = down + scal_ref[SUM_DOWN, base + z] * row
    for k, pay in enumerate(pays, 1):
        pay[...] = jnp.where(ids_ref[1] + k < len(pays) + 1, up, down)


def cyclic(size, k, stride=1):
    groups = size // stride
    return [
        (c * stride + r, ((c + k) % groups) * stride + r)
        for c in range(groups)
        for r in range(stride)
    ]


def update_kernel(
    ids_ref, scal_ref, t_ref, u_ref, edge_ref, keep_ref, back_ref, wide_ref,
    ylo_ref, yhi_ref, zlo_ref, zhi_ref, *rest, nz, final, resident,
):
    gots, corners, rest = rest[: nz - 1], rest[nz - 1 : 2 * nz - 2], rest[2 * nz - 2 :]
    if final:
        out_ref, e_ref, pq_ref = rest
    else:
        out_ref, nylo_ref, nyhi_ref, nzlo_ref, nzhi_ref, e_ref, pq_ref, s_ref = rest
    r = pl.program_id(0)
    depth, _, nx = t_ref.shape
    half = keep_ref.shape[1]
    tiles = wide_ref.shape[1] // SUB - 1
    scal = lambda i, j: scal_ref[i, j]

    @pl.when(r == 0)
    def _():
        core = lax.rem(ids_ref[0], 2)
        near = pl.multiple_of(core * half, SUB)
        far = pl.multiple_of((1 - core) * half, SUB)
        pq_ref[:, pl.ds(near, half), :] = keep_ref[...]
        pq_ref[:, pl.ds(far, half), :] = back_ref[...]

    own = pl.ds(pl.multiple_of(r * SUB, SUB), SUB)
    lo = wide_rows(wide_ref, (0, own), nx)
    hi = wide_rows(wide_ref, (1, own), nx)

    def solve(carry_rows, get_t, put_first, put_second):
        low = jnp.zeros((SUB, nx), f32)
        high = jnp.zeros((SUB, nx), f32)
        for k in range(1, nz):
            value = carry_rows(gots[k - 1])
            value = value + lo * corners[k - 1][0:1, :] + hi * corners[k - 1][1:2, :]
            low = low + scal(LINES, k) * value
            high = high + scal(LINES, FAR + k) * value

        def forward(z, carry):
            v = get_t(z) + lo * pq_ref[0, pl.ds(z, 1), :] + hi * pq_ref[1, pl.ds(z, 1), :]
            e = scal(DIAG, z) * v
            e_ref[z] = e
            s = carry + e
            put_first(z, s)
            return scal(UP, z) * s

        above = lax.fori_loop(0, depth, forward, scal(MISC, Z_LOW) * low, unroll=4)

        def backward(k, carry):
            z = depth - 1 - k
            put_second(z, carry)
            return scal(DOWN, z) * (carry + e_ref[z])

        below = lax.fori_loop(0, depth, backward, scal(MISC, Z_HIGH) * high, unroll=4)
        return low + below, high + above

    u_own = own if resident else slice(None)
    out_own = slice(None) if final else own

    def first(z, s):
        out_ref[z, out_own, :] = u_ref[z, u_own, :] + s

    def second(z, b):
        out_ref[z, out_own, :] = out_ref[z, out_own, :] + b

    @pl.when(r < tiles)
    def _():
        below, above = solve(lambda got: got[own, :], lambda z: t_ref[z, own, :], first, second)
        if not final:
            nzlo_ref[...] = zlo_ref[...] + below
            nzhi_ref[...] = zhi_ref[...] + above

    if not final:
        y_low = scal(MISC, Y_LOW)
        y_high = scal(MISC, Y_HIGH)
        pad = jnp.zeros((SUB - 2, nx), f32)

        def ends(got):
            rows = got.shape[0]
            return jnp.concatenate(
                [y_low * got[0:1, :], y_high * got[rows - 1 : rows, :], pad], axis=0
            )

        def keep_sum(z, s):
            s_ref[z] = s

        def put(z, b):
            value = s_ref[z] + b
            nylo_ref[pl.ds(z, 1), :] = ylo_ref[pl.ds(z, 1), :] + value[0:1]
            nyhi_ref[pl.ds(z, 1), :] = yhi_ref[pl.ds(z, 1), :] + value[1:2]

        @pl.when(r == tiles)
        def _():
            solve(ends, lambda z: edge_ref[z], keep_sum, put)


def update(ids, scal, t, u, edge, keep, back, wide, halos, gots, corners, final, resident):
    depth, rows, nx = u.shape
    nz = lax.axis_size("gz")
    tiles = rows // SUB
    ylo, yhi, zlo, zhi = halos
    clamp = lambda r: jnp.minimum(r, tiles - 1)
    field = pl.BlockSpec((depth, SUB, nx), lambda r: (0, clamp(r), 0))
    tile = pl.BlockSpec((SUB, nx), lambda r: (clamp(r), 0))
    outs = [shape(depth, rows, nx)]
    out_specs = [field if final else VMEM_WHOLE]
    scratch = [pltpu.VMEM((depth, SUB, nx), f32), pltpu.VMEM((2, depth, nx), f32)]
    if not final:
        outs += [shape(depth, nx)] * 2 + [shape(rows, nx)] * 2
        out_specs += [full(ylo), full(yhi), tile, tile]
        scratch += [pltpu.VMEM((depth, SUB, nx), f32)]
    return call(
        functools.partial(update_kernel, nz=nz, final=final, resident=resident),
        outs,
        (ids, scal, t, u, edge, keep, back, wide, ylo, yhi, zlo, zhi, *gots, *corners),
        grid=(tiles if final else tiles + 1,),
        in_specs=[
            smem(), smem(), VMEM_WHOLE, VMEM_WHOLE if resident else field, full(edge), full(keep), full(back), full(wide),
            full(ylo), full(yhi), tile, tile,
            *map(full, gots), *map(full, corners),
        ],
        out_specs=out_specs,
        scratch_shapes=scratch,
        resident=() if final else (0,),
        vmem=VL2,
        name="update",
    )


def halo(u):
    ny, nz = lax.axis_size("gy"), lax.axis_size("gz")
    up = lambda n: [(i, i + 1) for i in range(n - 1)]
    down = lambda n: [(i + 1, i) for i in range(n - 1)]
    ylo = lax.ppermute(u[:, -1, :], "gy", up(ny))
    yhi = lax.ppermute(u[:, 0, :], "gy", down(ny))
    zlo = lax.ppermute(u[-1], "gz", up(nz))
    zhi = lax.ppermute(u[0], "gz", down(nz))
    return ylo, yhi, zlo, zhi


def body(phase_field, others, cond_x, cond_y, cond_z, inverse_x, inverse_y, inverse_z):
    depth, rows, nx = phase_field.shape
    ny, nz = lax.axis_size("gy"), lax.axis_size("gz")
    half = depth // 2
    ids = jnp.stack([lax.axis_index("gy"), lax.axis_index("gz")])
    halos = halo(phase_field)
    *tabs, scal = tables(
        ids, inverse_x, inverse_y, inverse_z, cond_y, cond_z, rows, depth
    )
    wide = tabs[4]
    cx = jnp.pad(cond_x, (0, 1))[None]
    swap = [(i, i ^ 1) for i in range(ny)]
    u = phase_field
    for step in range(STEPS):
        final = step == STEPS - 1
        t, edge, mine, theirs, *pays = explicit(
            ids, scal, u, others, halos, tabs, cx, step > 0
        )
        gots = []
        for k in range(1, nz):
            gots.append(lax.ppermute(pays[k - 1], "gz", cyclic(nz, k)))
        other = lax.ppermute(theirs, "gy", swap)
        pays = call(
            chip_kernel,
            [shape(half, nx)] * (ny // 2 - 1),
            (ids, scal, mine, other),
            in_specs=[smem(), smem(), full(mine), full(other)],
            name="chip",
        )
        moved = [
            lax.ppermute(pays[k - 1], "gy", cyclic(ny, k, 2))
            for k in range(1, ny // 2)
        ]
        keep, give = call(
            share_kernel,
            [shape(2, half, nx)] * 2,
            (scal, mine, other, *moved),
            in_specs=[smem(), full(mine), full(other), *map(full, moved)],
            name="share",
        )
        back = lax.ppermute(give, "gy", swap)
        pays = call(
            corner_kernel,
            [shape(2, nx)] * (nz - 1),
            (ids, scal, keep, back),
            in_specs=[smem(), smem(), full(keep), full(back)],
            name="corner",
        )
        corners = [lax.ppermute(pays[k - 1], "gz", cyclic(nz, k)) for k in range(1, nz)]
        out = update(
            ids, scal, t, u, edge, keep, back, wide, halos, gots, corners,
            final, step > 0,
        )
        u, halos = out[0], out[1:]
    return u


def solution(mesh):
    placed = (P("gz", "gy", None), P("gz", "gy", None), P(), P(), P(), P(), P(), P())
    return jax.shard_map(
        body, mesh=mesh, in_specs=placed, out_specs=P("gz", "gy", None), check_vma=False
    )
```

```python
import functools

import jax
import jax.numpy as jnp
from jax import lax
from jax.experimental import pallas as pl
from jax.experimental.pallas import tpu as pltpu
from jax.sharding import PartitionSpec as P


STEPS = 2
REACTION = 2.0
LANES = 128
SUB = 8
XB = 256
ZB = 8
PAIR = 2
VL1 = 30
VL2 = 20

DIAG, UP, DOWN, SUM_UP, SUM_DOWN, COND, MISC, CHIPS, LINES = range(9)
TABLE_ROWS = 16
Z_LOW, Z_HIGH, Y_LOW, Y_HIGH, MIX, KEEP, GIVE = 0, 1, 2, 3, 4, 8, 12
LARGE = 2**20
FAR = 64

f32 = jnp.float32
bf16 = jnp.bfloat16


def split(a):
    high = a.astype(bf16)
    low = (a - high.astype(f32)).astype(bf16)
    return high, low


def wide_rows(ref, rows, nx):
    return jnp.concatenate([ref[rows]] * (nx // LANES), axis=1)


VMEM_WHOLE = pl.BlockSpec(memory_space=pltpu.VMEM)


def full(a):
    return pl.BlockSpec(a.shape, lambda *_: (0,) * len(a.shape))


def smem():
    return pl.BlockSpec(memory_space=pltpu.SMEM)


def call(kernel, out_shape, operands, **kw):
    limit = kw.pop("vmem", 16)
    large = kw.pop("large", LARGE)
    resident = kw.pop("resident", ())
    operands = [
        pltpu.with_memory_space_constraint(a, pltpu.HBM)
        if a.size >= large and s is not VMEM_WHOLE
        else a
        for a, s in zip(operands, kw["in_specs"])
    ]
    out_shape = [
        pltpu.VMEM(a.shape, a.dtype)
        if i in resident
        else pltpu.HBM(a.shape, a.dtype)
        if a.size >= large
        else a
        for i, a in enumerate(out_shape)
    ]
    return pl.pallas_call(
        kernel,
        out_shape=out_shape,
        compiler_params=pltpu.CompilerParams(
            dimension_semantics=("arbitrary",) * len(kw.get("grid", ())),
            vmem_limit_bytes=limit * 2**20,
        ),
        **kw,
    )(*operands)


def shape(*dims, dtype=f32):
    return jax.ShapeDtypeStruct(dims, dtype)


def strip_of(ref, start, count):
    total = ref.shape[0]
    top = pl.multiple_of(lax.rem(start - SUB + total, total), SUB)
    end = pl.multiple_of(lax.rem(start + count, total), SUB)
    rows = jnp.concatenate(
        [
            ref[pl.ds(top, SUB), :],
            ref[pl.ds(pl.multiple_of(start, SUB), count), :],
            ref[pl.ds(end, SUB), :],
        ],
        axis=0,
    )
    return pltpu.roll(rows, lax.rem(total - start, total), 1)


def entry(ref, i, j):
    total = ref.shape[0]
    i = lax.rem(i + total, total)
    j = lax.rem(j + total, total)
    row = ref[pl.ds(i, 1), :]
    lane = lax.broadcasted_iota(jnp.int32, row.shape, 1)
    return jnp.sum(jnp.where(lane == j, row, 0.0), axis=1, keepdims=True)


def over_pivot(ref, i, j):
    return entry(ref, i, j) / entry(ref, j, j)


def tables_kernel(
    ids_ref, ax_ref, lower_ref, lpiv_ref, upper_ref, upiv_ref, ay_ref, az_ref,
    cond_ref,
    axh_ref, axl_ref, xlo_ref, xhi_ref, wide_ref, mat_ref, scal_ref,
    *, rows, depth, ny, nz, widths,
):
    nx, wy, wz = widths
    e = pl.program_id(0)
    last = pl.num_programs(0) - 1
    high, low = split(ax_ref[...].T)
    axh_ref[e] = high
    axl_ref[e] = low
    cols = pl.ds(pl.multiple_of(e * XB, XB), XB)
    from_low = lower_ref[...].T[LANES - 1 :] / lpiv_ref[SUB - 1 :, LANES - 1 :]
    from_high = upper_ref[...].T[:1] / upiv_ref[:1, :1]
    xlo_ref[:, cols] = jnp.where(e > 0, from_low, 0.0)
    xhi_ref[:, cols] = jnp.where(e < last, from_high, 0.0)

    @pl.when(e == 0)
    def _():
        gy, gz = ids_ref[0], ids_ref[1]
        y0, z0 = gy * rows, gz * depth
        ys = strip_of(ay_ref, y0, rows)
        zs = strip_of(az_ref, z0, depth)
        end = ay_ref.shape[0] - 1
        pad = jnp.zeros((SUB - 2, 1), f32)

        def arranged(column):
            return jnp.concatenate(
                [
                    column[SUB : SUB + rows],
                    column[SUB - 1 : SUB],
                    column[SUB + rows : SUB + rows + 1],
                    pad,
                ],
                axis=0,
            )

        lo = arranged(ys[:, end:] / ys[SUB - 1 : SUB, end:])
        hi = arranged(
            ys[:, rows : rows + 1] / ys[SUB + rows : SUB + rows + 1, rows : rows + 1]
        )
        wide_ref[0] = jnp.broadcast_to(lo, (rows + SUB, LANES))
        wide_ref[1] = jnp.broadcast_to(hi, (rows + SUB, LANES))
        cy = pltpu.roll(cond_ref[:, nx : nx + wy], lax.rem(wy - y0, wy), 1)
        cy = jnp.broadcast_to(cy[:, :LANES], (LANES, LANES)).T
        wide_ref[2] = cy[1 : rows + 1 + SUB]
        wide_ref[3] = cy[: rows + SUB]
        bh, bl = split(ys[SUB : SUB + rows, :rows])
        mat_ref[:rows, :] = jnp.concatenate([bh, bh], axis=1)
        mat_ref[rows:, :] = jnp.concatenate([bl, jnp.zeros_like(bl)], axis=1)

        total = az_ref.shape[0]
        r = lax.broadcasted_iota(jnp.int32, zs.shape, 0)
        c = lax.broadcasted_iota(jnp.int32, zs.shape, 1)
        pick = lambda shift: jnp.sum(
            jnp.where(r == c + (SUB + shift), zs, 0.0), axis=0, keepdims=True
        )
        lane = lax.broadcasted_iota(jnp.int32, (1, total), 1)
        diag = jnp.where(lane < depth, pick(0), 1.0)
        scal_ref[...] = jnp.zeros_like(scal_ref)

        def row(index, value):
            scal_ref[index : index + 1, :] = value[:, :LANES]

        row(DIAG, diag)
        row(UP, pick(1) / diag)
        row(DOWN, pick(-1) / diag)
        row(SUM_UP, zs[SUB + depth - 1 : SUB + depth])
        row(SUM_DOWN, zs[SUB : SUB + 1])
        cz = pltpu.roll(cond_ref[:, nx + wy :], lax.rem(wz - z0, wz), 1)
        row(COND, cz)

        lane = lax.broadcasted_iota(jnp.int32, (1, LANES), 1)

        def fill(index, values):
            line = jnp.zeros((1, LANES), f32)
            for at, value in values.items():
                line = jnp.where(lane == at, value, line)
            row(index, line)

        far = total - 1
        core = lax.rem(gy, 2)
        chip = gy // 2
        chips = ny // 2
        yb = chip * (2 * rows)
        one = jnp.ones((1, 1), f32)
        zero = jnp.zeros((1, 1), f32)
        up = over_pivot(ay_ref, yb + 2 * rows - 1, yb + rows - 1)
        down = over_pivot(ay_ref, yb, yb + rows)
        through_up = over_pivot(ay_ref, yb + rows - 1, yb - 1)
        through_down = over_pivot(ay_ref, yb + rows, yb + 2 * rows)
        by_core = lambda a, b: jnp.where(core == 0, a, b)
        fill(
            MISC,
            {
                Z_LOW: zs[SUB : SUB + 1, far:] / zs[SUB - 1 : SUB, far:],
                Z_HIGH: zs[SUB + depth - 1 : SUB + depth, depth : depth + 1]
                / zs[SUB + depth : SUB + depth + 1, depth : depth + 1],
                Y_LOW: ys[SUB - 1 : SUB, :1] / ys[SUB : SUB + 1, :1],
                Y_HIGH: ys[SUB + rows : SUB + rows + 1, rows - 1 : rows]
                / ys[SUB + rows - 1 : SUB + rows, rows - 1 : rows],
                MIX: by_core(up, one),
                MIX + 1: by_core(one, up),
                MIX + 2: by_core(one, down),
                MIX + 3: by_core(down, one),
                KEEP: by_core(one, through_up),
                KEEP + 1: by_core(zero, one),
                KEEP + 2: by_core(through_down, one),
                KEEP + 3: by_core(one, zero),
                GIVE: by_core(through_up, one),
                GIVE + 1: by_core(one, zero),
                GIVE + 2: by_core(one, through_down),
                GIVE + 3: by_core(zero, one),
            },
        )
        values = {}
        for k in range(1, chips):
            src = lax.rem(chip - k + chips, chips)
            below = src < chip
            a = over_pivot(ay_ref, yb - 1, (src + 1) * 2 * rows - 1)
            b = over_pivot(ay_ref, yb + 2 * rows, src * 2 * rows)
            values[k] = jnp.where(below, a, 0.0)
            values[FAR + k] = jnp.where(below, 0.0, b)
        fill(CHIPS, values)
        values = {}
        for k in range(1, nz):
            src = lax.rem(gz - k + nz, nz)
            below = src < gz
            a = over_pivot(az_ref, z0 - 1, (src + 1) * depth - 1)
            b = over_pivot(az_ref, z0 + depth, src * depth)
            values[k] = jnp.where(below, a, 0.0)
            values[FAR + k] = jnp.where(below, 0.0, b)
        fill(LINES, values)


def tables(ids, inverse_x, inverse_y, inverse_z, conds, widths, rows, depth):
    nx = inverse_x.shape[0]
    blocks = nx // XB
    ny, nz = lax.axis_size("gy"), lax.axis_size("gz")
    q, s = XB // LANES, XB // SUB
    column = lambda at: pl.BlockSpec((XB, LANES), lambda e: (e, at(e)))
    low = lambda e: jnp.maximum(q * e - 1, 0)
    top = lambda e: jnp.minimum(q * e + q, q * blocks - 1)
    return call(
        functools.partial(
            tables_kernel, rows=rows, depth=depth, ny=ny, nz=nz, widths=widths
        ),
        [
            shape(blocks, XB, XB, dtype=bf16),
            shape(blocks, XB, XB, dtype=bf16),
            shape(1, nx),
            shape(1, nx),
            shape(4, rows + SUB, LANES),
            shape(2 * rows, 2 * rows, dtype=bf16),
            shape(TABLE_ROWS, LANES),
        ],
        (ids, inverse_x, inverse_x, inverse_x, inverse_x, inverse_x, inverse_y, inverse_z, conds),
        grid=(blocks,),
        in_specs=[
            smem(),
            pl.BlockSpec((XB, XB), lambda e: (e, e)),
            column(low),
            pl.BlockSpec((SUB, LANES), lambda e: (jnp.maximum(s * e - 1, 0), low(e))),
            column(top),
            pl.BlockSpec(
                (SUB, LANES), lambda e: (jnp.minimum(s * e + s, s * blocks - 1), top(e))
            ),
            full(inverse_y), full(inverse_z), full(conds),
        ],
        out_specs=[
            *[VMEM_WHOLE] * 6,
            full(shape(TABLE_ROWS, LANES)),
        ],
        resident=range(6),
        large=2**14,
        name="tables",
    )


def explicit_kernel(
    ids_ref, scal_ref, *rest, nz, resident,
):
    if resident:
        u_ref, *rest = rest
    else:
        u_ref, above_ref, *rest = rest
    o_ref, ylo_ref, yhi_ref, zlo_ref, zhi_ref, cx_ref, wide_ref, *rest = rest
    ay_ref, axh_ref, axl_ref, xlo_ref, xhi_ref, *rest = rest
    t_ref, edge_ref, mine_ref, theirs_ref, *rest = rest
    pays = rest[: nz - 1]
    even_ref, odd_ref, line_ref, other_ref, sy_ref, sz_ref, high_ref, flux_ref = rest[
        nz - 1 :
    ]
    step = pl.program_id(0)
    steps = pl.num_programs(0)
    zb, rows, nx = o_ref.shape
    tiles = rows // SUB
    blocks = nx // XB
    base_z = step * zb if resident else 0
    sub = lax.broadcasted_iota(jnp.int32, (SUB, nx), 0)
    dot = functools.partial(jnp.dot, preferred_element_type=f32)

    over = u_ref[jnp.minimum(base_z + zb, steps * zb - 1)] if resident else above_ref[0]
    high_ref[...] = jnp.where(step < steps - 1, over, zhi_ref[...])

    @pl.when(step == 0)
    def _():
        sz_ref[...] = jnp.zeros_like(sz_ref)
        odd_ref[...] = jnp.zeros_like(odd_ref)
        flux_ref[...] = (u_ref[0] - zlo_ref[...]) * scal_ref[COND, 0]

    def plane(z, out_ref):
        zz = step * zb + z
        c_up = scal_ref[COND, zz + 1]
        cx = jnp.broadcast_to(cx_ref[:, :nx], (SUB, nx))

        def get(r):
            return u_ref[base_z + z, r * SUB : (r + 1) * SUB, :]

        current = get(0)
        first = current[:1] - ylo_ref[pl.ds(zz, 1), :]
        first = first * wide_rows(wide_ref, (3, slice(0, 1)), nx)
        before = jnp.broadcast_to(first, (SUB, nx))
        for r in range(tiles):
            own = slice(r * SUB, (r + 1) * SUB)
            c = current
            if r + 1 < tiles:
                current = get(r + 1)
                up_next = pltpu.roll(current, SUB - 1, 0)
            else:
                up_next = jnp.broadcast_to(yhi_ref[pl.ds(zz, 1), :], (SUB, nx))
            up = jnp.where(sub == SUB - 1, up_next, pltpu.roll(c, SUB - 1, 0))
            fx = (pltpu.roll(c, nx - 1, 1) - c) * cx
            total = fx - pltpu.roll(fx, 1, 1)
            fy = (up - c) * wide_rows(wide_ref, (2, own), nx)
            rolled = pltpu.roll(fy, 1, 0)
            total = total + (fy - jnp.where(sub == 0, before, rolled))
            before = rolled
            above = high_ref[own, :] if z == zb - 1 else u_ref[base_z + z + 1, own, :]
            fz = (above - c) * c_up
            total = total + (fz - flux_ref[own, :])
            flux_ref[own, :] = fz
            o = o_ref[z, own, :]
            total = total + (REACTION * c) * (1.0 - c * c - 2.0 * o)
            at = (z % PAIR) * rows + r * SUB
            out_ref[at : at + SUB, :] = total

    y_low = scal_ref[MISC, Y_LOW]
    y_high = scal_ref[MISC, Y_HIGH]

    def solves(first, in_ref, x_ref):
        for e in range(blocks):
            cols = slice(e * XB, (e + 1) * XB)
            high, low = split(in_ref[:, cols])
            x_ref[:, cols] = (
                dot(high, axh_ref[e]) + dot(low, axh_ref[e]) + dot(high, axl_ref[e])
            )
        lows = [None]
        for e in range(blocks - 1):
            at = slice((e + 1) * XB - 1, (e + 1) * XB)
            end = x_ref[:, at]
            if lows[e] is not None:
                end = end + lows[e] * xlo_ref[:, at]
            lows.append(end)
        highs = [None] * blocks
        for e in reversed(range(1, blocks)):
            at = slice(e * XB, e * XB + 1)
            end = x_ref[:, at]
            if highs[e] is not None:
                end = end + highs[e] * xhi_ref[:, at]
            highs[e - 1] = end
        for e in range(blocks):
            cols = slice(e * XB, (e + 1) * XB)
            up_sum = sz_ref[0, :, cols]
            down_sum = sz_ref[1, :, cols]
            for i in range(PAIR):
                zz = jnp.maximum(first + i, 0)
                here = slice(i * rows, (i + 1) * rows)
                value = x_ref[here, cols]
                if lows[e] is not None:
                    value = value + lows[e][here] * xlo_ref[:, cols]
                if highs[e] is not None:
                    value = value + highs[e][here] * xhi_ref[:, cols]
                high, low = split(value)
                result = dot(ay_ref[...], jnp.concatenate([high, low], axis=0))
                value = result[:rows] + result[rows:]
                t_ref[zz, :, cols] = value
                bottom, top = value[:1], value[rows - 1 :]
                sy_ref[0, pl.ds(zz, 1), cols] = top
                sy_ref[1, pl.ds(zz, 1), cols] = bottom
                edge_ref[zz, 0:1, cols] = y_low * bottom
                edge_ref[zz, 1:2, cols] = y_high * top
                up_sum = up_sum + scal_ref[SUM_UP, zz] * value
                down_sum = down_sum + scal_ref[SUM_DOWN, zz] * value
            sz_ref[0, :, cols] = up_sum
            sz_ref[1, :, cols] = down_sum

    parity = [(even_ref, line_ref), (odd_ref, other_ref)]
    for k in range(zb // PAIR):
        for i in range(PAIR):
            plane(k * PAIR + i, parity[k % 2][0])
        solves(step * zb + (k - 1) * PAIR, *parity[(k - 1) % 2])

    @pl.when(step == steps - 1)
    def _():
        solves(step * zb + zb - PAIR, *parity[(zb // PAIR - 1) % 2])
        half = mine_ref.shape[1]
        core = lax.rem(ids_ref[0], 2)
        near = pl.multiple_of(core * half, SUB)
        far = pl.multiple_of((1 - core) * half, SUB)
        mine_ref[...] = sy_ref[:, pl.ds(near, half), :]
        theirs_ref[...] = sy_ref[:, pl.ds(far, half), :]
        for k in range(1, nz):
            higher = ids_ref[1] + k < nz
            pays[k - 1][...] = jnp.where(higher, sz_ref[0], sz_ref[1])


def explicit(ids, scal, u, o, halos, tabs, cx, resident):
    depth, rows, nx = u.shape
    axh, axl, xlo, xhi, wide, mat = tabs
    nz = lax.axis_size("gz")
    zb = ZB
    steps = depth // zb
    half = depth // 2
    field = pl.BlockSpec((zb, rows, nx), lambda s: (s, 0, 0))
    above = pl.BlockSpec(
        (1, rows, nx), lambda s: (jnp.minimum(s * zb + zb, depth - 1), 0, 0)
    )
    rest = (*halos, cx, wide, mat, axh, axl, xlo, xhi)
    outs = [
        shape(depth, rows, nx),
        shape(depth, SUB, nx),
        shape(2, half, nx),
        shape(2, half, nx),
    ] + [shape(rows, nx)] * (nz - 1)
    return call(
        functools.partial(explicit_kernel, nz=nz, resident=resident),
        outs,
        (ids, scal, *([u] if resident else [u, u]), o, *rest),
        grid=(steps,),
        in_specs=[smem(), smem()]
        + ([VMEM_WHOLE] if resident else [field, above])
        + [field, *map(full, halos), full(cx), *[VMEM_WHOLE] * 6],
        resident=(0, 1),
        out_specs=[VMEM_WHOLE, VMEM_WHOLE] + [full(a) for a in outs[2:]],
        scratch_shapes=[pltpu.VMEM((PAIR * rows, nx), f32)] * 4
        + [
            pltpu.VMEM((2, depth, nx), f32),
            pltpu.VMEM((2, rows, nx), f32),
            pltpu.VMEM((rows, nx), f32),
            pltpu.VMEM((rows, nx), f32),
        ],
        vmem=VL1,
        name="explicit",
    )


def chip_kernel(ids_ref, scal_ref, mine_ref, other_ref, *pays):
    mix = lambda i: scal_ref[MISC, MIX + i]
    up = mix(0) * mine_ref[0] + mix(1) * other_ref[0]
    down = mix(2) * mine_ref[1] + mix(3) * other_ref[1]
    chip = ids_ref[0] // 2
    for k, pay in enumerate(pays, 1):
        pay[...] = jnp.where(chip + k < len(pays) + 1, up, down)


def share_kernel(scal_ref, mine_ref, other_ref, *rest):
    *gots, keep_ref, give_ref = rest
    low = jnp.zeros_like(gots[0])
    high = jnp.zeros_like(gots[0])
    for k, got in enumerate(gots, 1):
        low = low + scal_ref[CHIPS, k] * got[...]
        high = high + scal_ref[CHIPS, FAR + k] * got[...]
    keep = lambda i: scal_ref[MISC, KEEP + i]
    give = lambda i: scal_ref[MISC, GIVE + i]
    keep_ref[0] = keep(0) * low + keep(1) * other_ref[0]
    keep_ref[1] = keep(2) * high + keep(3) * other_ref[1]
    give_ref[0] = give(0) * low + give(1) * mine_ref[0]
    give_ref[1] = give(2) * high + give(3) * mine_ref[1]


def corner_kernel(ids_ref, scal_ref, keep_ref, back_ref, *pays):
    half = keep_ref.shape[1]
    core = lax.rem(ids_ref[0], 2)
    near, far = core * half, (1 - core) * half
    up = jnp.zeros((2, keep_ref.shape[2]), f32)
    down = jnp.zeros_like(up)
    for z in range(half):
        for ref, base in ((keep_ref, near), (back_ref, far)):
            row = ref[:, z, :]
            up = up + scal_ref[SUM_UP, base + z] * row
            down = down + scal_ref[SUM_DOWN, base + z] * row
    for k, pay in enumerate(pays, 1):
        pay[...] = jnp.where(ids_ref[1] + k < len(pays) + 1, up, down)


def cyclic(size, k, stride=1):
    groups = size // stride
    return [
        (c * stride + r, ((c + k) % groups) * stride + r)
        for c in range(groups)
        for r in range(stride)
    ]


def update_kernel(
    ids_ref, scal_ref, t_ref, u_ref, edge_ref, keep_ref, back_ref, wide_ref,
    ylo_ref, yhi_ref, zlo_ref, zhi_ref, *rest, nz, final, resident,
):
    gots, corners, rest = rest[: nz - 1], rest[nz - 1 : 2 * nz - 2], rest[2 * nz - 2 :]
    if final:
        out_ref, e_ref, pq_ref = rest
    else:
        out_ref, nylo_ref, nyhi_ref, nzlo_ref, nzhi_ref, e_ref, pq_ref, s_ref = rest
    r = pl.program_id(0)
    depth, _, nx = t_ref.shape
    half = keep_ref.shape[1]
    tiles = wide_ref.shape[1] // SUB - 1
    scal = lambda i, j: scal_ref[i, j]

    @pl.when(r == 0)
    def _():
        core = lax.rem(ids_ref[0], 2)
        near = pl.multiple_of(core * half, SUB)
        far = pl.multiple_of((1 - core) * half, SUB)
        pq_ref[:, pl.ds(near, half), :] = keep_ref[...]
        pq_ref[:, pl.ds(far, half), :] = back_ref[...]

    own = pl.ds(pl.multiple_of(r * SUB, SUB), SUB)
    lo = wide_rows(wide_ref, (0, own), nx)
    hi = wide_rows(wide_ref, (1, own), nx)

    def solve(carry_rows, get_t, put_first, put_second):
        low = jnp.zeros((SUB, nx), f32)
        high = jnp.zeros((SUB, nx), f32)
        for k in range(1, nz):
            value = carry_rows(gots[k - 1])
            value = value + lo * corners[k - 1][0:1, :] + hi * corners[k - 1][1:2, :]
            low = low + scal(LINES, k) * value
            high = high + scal(LINES, FAR + k) * value

        def forward(z, carry):
            v = get_t(z) + lo * pq_ref[0, pl.ds(z, 1), :] + hi * pq_ref[1, pl.ds(z, 1), :]
            e = scal(DIAG, z) * v
            e_ref[z] = e
            s = carry + e
            put_first(z, s)
            return scal(UP, z) * s

        above = lax.fori_loop(0, depth, forward, scal(MISC, Z_LOW) * low, unroll=4)

        def backward(k, carry):
            z = depth - 1 - k
            put_second(z, carry)
            return scal(DOWN, z) * (carry + e_ref[z])

        below = lax.fori_loop(0, depth, backward, scal(MISC, Z_HIGH) * high, unroll=4)
        return low + below, high + above

    u_own = own if resident else slice(None)
    out_own = slice(None) if final else own

    def first(z, s):
        out_ref[z, out_own, :] = u_ref[z, u_own, :] + s

    def second(z, b):
        out_ref[z, out_own, :] = out_ref[z, out_own, :] + b

    @pl.when(r < tiles)
    def _():
        below, above = solve(lambda got: got[own, :], lambda z: t_ref[z, own, :], first, second)
        if not final:
            nzlo_ref[...] = zlo_ref[...] + below
            nzhi_ref[...] = zhi_ref[...] + above

    if not final:
        y_low = scal(MISC, Y_LOW)
        y_high = scal(MISC, Y_HIGH)
        pad = jnp.zeros((SUB - 2, nx), f32)

        def ends(got):
            rows = got.shape[0]
            return jnp.concatenate(
                [y_low * got[0:1, :], y_high * got[rows - 1 : rows, :], pad], axis=0
            )

        def keep_sum(z, s):
            s_ref[z] = s

        def put(z, b):
            value = s_ref[z] + b
            nylo_ref[pl.ds(z, 1), :] = ylo_ref[pl.ds(z, 1), :] + value[0:1]
            nyhi_ref[pl.ds(z, 1), :] = yhi_ref[pl.ds(z, 1), :] + value[1:2]

        @pl.when(r == tiles)
        def _():
            solve(ends, lambda z: edge_ref[z], keep_sum, put)


def update(ids, scal, t, u, edge, keep, back, wide, halos, gots, corners, final, resident):
    depth, rows, nx = u.shape
    nz = lax.axis_size("gz")
    tiles = rows // SUB
    ylo, yhi, zlo, zhi = halos
    clamp = lambda r: jnp.minimum(r, tiles - 1)
    field = pl.BlockSpec((depth, SUB, nx), lambda r: (0, clamp(r), 0))
    tile = pl.BlockSpec((SUB, nx), lambda r: (clamp(r), 0))
    outs = [shape(depth, rows, nx)]
    out_specs = [field if final else VMEM_WHOLE]
    scratch = [pltpu.VMEM((depth, SUB, nx), f32), pltpu.VMEM((2, depth, nx), f32)]
    if not final:
        outs += [shape(depth, nx)] * 2 + [shape(rows, nx)] * 2
        out_specs += [full(ylo), full(yhi), tile, tile]
        scratch += [pltpu.VMEM((depth, SUB, nx), f32)]
    return call(
        functools.partial(update_kernel, nz=nz, final=final, resident=resident),
        outs,
        (ids, scal, t, u, edge, keep, back, wide, ylo, yhi, zlo, zhi, *gots, *corners),
        grid=(tiles if final else tiles + 1,),
        in_specs=[
            smem(), smem(), VMEM_WHOLE, VMEM_WHOLE if resident else field, VMEM_WHOLE, full(keep), full(back), full(wide),
            full(ylo), full(yhi), tile, tile,
            *map(full, gots), *map(full, corners),
        ],
        out_specs=out_specs,
        scratch_shapes=scratch,
        resident=() if final else (0,),
        vmem=VL2,
        name="update",
    )


def halo(u):
    ny, nz = lax.axis_size("gy"), lax.axis_size("gz")
    up = lambda n: [(i, i + 1) for i in range(n - 1)]
    down = lambda n: [(i + 1, i) for i in range(n - 1)]
    ylo = lax.ppermute(u[:, -1, :], "gy", up(ny))
    yhi = lax.ppermute(u[:, 0, :], "gy", down(ny))
    zlo = lax.ppermute(u[-1], "gz", up(nz))
    zhi = lax.ppermute(u[0], "gz", down(nz))
    return ylo, yhi, zlo, zhi


def body(phase_field, others, cond_x, cond_y, cond_z, inverse_x, inverse_y, inverse_z):
    depth, rows, nx = phase_field.shape
    ny, nz = lax.axis_size("gy"), lax.axis_size("gz")
    half = depth // 2
    ids = jnp.stack([lax.axis_index("gy"), lax.axis_index("gz")])
    halos = halo(phase_field)
    room = lambda n: -(-(n + 3 + LANES) // LANES) * LANES
    wy, wz = room(cond_y.shape[0]), room(cond_z.shape[0])
    conds = jnp.concatenate(
        [
            jnp.pad(cond_x, (0, 1)),
            jnp.pad(cond_y, (1, wy - 1 - cond_y.shape[0])),
            jnp.pad(cond_z, (1, wz - 1 - cond_z.shape[0])),
        ]
    )[None]
    *tabs, scal = tables(
        ids, inverse_x, inverse_y, inverse_z, conds, (nx, wy, wz), rows, depth
    )
    wide = tabs[4]
    cx = conds
    swap = [(i, i ^ 1) for i in range(ny)]
    u = phase_field
    for step in range(STEPS):
        final = step == STEPS - 1
        t, edge, mine, theirs, *pays = explicit(
            ids, scal, u, others, halos, tabs, cx, step > 0
        )
        gots = []
        for k in range(1, nz):
            gots.append(lax.ppermute(pays[k - 1], "gz", cyclic(nz, k)))
        other = lax.ppermute(theirs, "gy", swap)
        pays = call(
            chip_kernel,
            [shape(half, nx)] * (ny // 2 - 1),
            (ids, scal, mine, other),
            in_specs=[smem(), smem(), full(mine), full(other)],
            name="chip",
        )
        moved = [
            lax.ppermute(pays[k - 1], "gy", cyclic(ny, k, 2))
            for k in range(1, ny // 2)
        ]
        keep, give = call(
            share_kernel,
            [shape(2, half, nx)] * 2,
            (scal, mine, other, *moved),
            in_specs=[smem(), full(mine), full(other), *map(full, moved)],
            name="share",
        )
        back = lax.ppermute(give, "gy", swap)
        pays = call(
            corner_kernel,
            [shape(2, nx)] * (nz - 1),
            (ids, scal, keep, back),
            in_specs=[smem(), smem(), full(keep), full(back)],
            name="corner",
        )
        corners = [lax.ppermute(pays[k - 1], "gz", cyclic(nz, k)) for k in range(1, nz)]
        out = update(
            ids, scal, t, u, edge, keep, back, wide, halos, gots, corners,
            final, step > 0,
        )
        u, halos = out[0], out[1:]
    return u


def solution(mesh):
    placed = (P("gz", "gy", None), P("gz", "gy", None), P(), P(), P(), P(), P(), P())
    return jax.shard_map(
        body, mesh=mesh, in_specs=placed, out_specs=P("gz", "gy", None), check_vma=False
    )
```

```python
import functools

import jax
import jax.numpy as jnp
from jax import lax
from jax.experimental import pallas as pl
from jax.experimental.pallas import tpu as pltpu
from jax.sharding import PartitionSpec as P


STEPS = 2
REACTION = 2.0
LANES = 128
SUB = 8
XB = 256
ZB = 8
YU = 8
PAIR = 1
VL1 = 30
VL2 = 20

DIAG, UP, DOWN, SUM_UP, SUM_DOWN, COND, MISC, CHIPS, LINES = range(9)
TABLE_ROWS = 16
Z_LOW, Z_HIGH, Y_LOW, Y_HIGH, MIX, KEEP, GIVE = 0, 1, 2, 3, 4, 8, 12
LARGE = 2**20
FAR = 64

f32 = jnp.float32
bf16 = jnp.bfloat16


def split(a):
    high = a.astype(bf16)
    low = (a - high.astype(f32)).astype(bf16)
    return high, low


def wide_rows(ref, rows, nx):
    return jnp.concatenate([ref[rows]] * (nx // LANES), axis=1)


VMEM_WHOLE = pl.BlockSpec(memory_space=pltpu.VMEM)


def full(a):
    return pl.BlockSpec(a.shape, lambda *_: (0,) * len(a.shape))


def smem():
    return pl.BlockSpec(memory_space=pltpu.SMEM)


def call(kernel, out_shape, operands, **kw):
    limit = kw.pop("vmem", 16)
    large = kw.pop("large", LARGE)
    resident = kw.pop("resident", ())
    operands = [
        pltpu.with_memory_space_constraint(a, pltpu.HBM)
        if a.size >= large and s is not VMEM_WHOLE
        else a
        for a, s in zip(operands, kw["in_specs"])
    ]
    out_shape = [
        pltpu.VMEM(a.shape, a.dtype)
        if i in resident
        else pltpu.HBM(a.shape, a.dtype)
        if a.size >= large
        else a
        for i, a in enumerate(out_shape)
    ]
    return pl.pallas_call(
        kernel,
        out_shape=out_shape,
        compiler_params=pltpu.CompilerParams(
            dimension_semantics=("arbitrary",) * len(kw.get("grid", ())),
            vmem_limit_bytes=limit * 2**20,
        ),
        **kw,
    )(*operands)


def shape(*dims, dtype=f32):
    return jax.ShapeDtypeStruct(dims, dtype)


def strip_of(ref, start, count):
    total = ref.shape[0]
    top = pl.multiple_of(lax.rem(start - SUB + total, total), SUB)
    end = pl.multiple_of(lax.rem(start + count, total), SUB)
    rows = jnp.concatenate(
        [
            ref[pl.ds(top, SUB), :],
            ref[pl.ds(pl.multiple_of(start, SUB), count), :],
            ref[pl.ds(end, SUB), :],
        ],
        axis=0,
    )
    return pltpu.roll(rows, lax.rem(total - start, total), 1)


def entry(ref, i, j):
    total = ref.shape[0]
    i = lax.rem(i + total, total)
    j = lax.rem(j + total, total)
    row = ref[pl.ds(i, 1), :]
    lane = lax.broadcasted_iota(jnp.int32, row.shape, 1)
    return jnp.sum(jnp.where(lane == j, row, 0.0), axis=1, keepdims=True)


def over_pivot(ref, i, j):
    return entry(ref, i, j) / entry(ref, j, j)


def tables_kernel(
    ids_ref, ax_ref, lower_ref, lpiv_ref, upper_ref, upiv_ref, ay_ref, az_ref,
    cond_ref,
    axh_ref, axl_ref, xlo_ref, xhi_ref, wide_ref, mat_ref, scal_ref,
    *, rows, depth, ny, nz, widths,
):
    nx, wy, wz = widths
    e = pl.program_id(0)
    last = pl.num_programs(0) - 1
    high, low = split(ax_ref[...].T)
    axh_ref[e] = high
    axl_ref[e] = low
    cols = pl.ds(pl.multiple_of(e * XB, XB), XB)
    from_low = lower_ref[...].T[LANES - 1 :] / lpiv_ref[SUB - 1 :, LANES - 1 :]
    from_high = upper_ref[...].T[:1] / upiv_ref[:1, :1]
    xlo_ref[:, cols] = jnp.where(e > 0, from_low, 0.0)
    xhi_ref[:, cols] = jnp.where(e < last, from_high, 0.0)

    @pl.when(e == 0)
    def _():
        gy, gz = ids_ref[0], ids_ref[1]
        y0, z0 = gy * rows, gz * depth
        ys = strip_of(ay_ref, y0, rows)
        zs = strip_of(az_ref, z0, depth)
        end = ay_ref.shape[0] - 1
        pad = jnp.zeros((SUB - 2, 1), f32)

        def arranged(column):
            return jnp.concatenate(
                [
                    column[SUB : SUB + rows],
                    column[SUB - 1 : SUB],
                    column[SUB + rows : SUB + rows + 1],
                    pad,
                ],
                axis=0,
            )

        lo = arranged(ys[:, end:] / ys[SUB - 1 : SUB, end:])
        hi = arranged(
            ys[:, rows : rows + 1] / ys[SUB + rows : SUB + rows + 1, rows : rows + 1]
        )
        wide_ref[0] = jnp.broadcast_to(lo, (rows + SUB, LANES))
        wide_ref[1] = jnp.broadcast_to(hi, (rows + SUB, LANES))
        cy = pltpu.roll(cond_ref[:, nx : nx + wy], lax.rem(wy - y0, wy), 1)
        cy = jnp.broadcast_to(cy[:, :LANES], (LANES, LANES)).T
        wide_ref[2] = cy[1 : rows + 1 + SUB]
        wide_ref[3] = cy[: rows + SUB]
        bh, bl = split(ys[SUB : SUB + rows, :rows])
        mat_ref[:rows, :] = jnp.concatenate([bh, bh], axis=1)
        mat_ref[rows:, :] = jnp.concatenate([bl, jnp.zeros_like(bl)], axis=1)

        total = az_ref.shape[0]
        r = lax.broadcasted_iota(jnp.int32, zs.shape, 0)
        c = lax.broadcasted_iota(jnp.int32, zs.shape, 1)
        pick = lambda shift: jnp.sum(
            jnp.where(r == c + (SUB + shift), zs, 0.0), axis=0, keepdims=True
        )
        lane = lax.broadcasted_iota(jnp.int32, (1, total), 1)
        diag = jnp.where(lane < depth, pick(0), 1.0)
        scal_ref[...] = jnp.zeros_like(scal_ref)

        def row(index, value):
            scal_ref[index : index + 1, :] = value[:, :LANES]

        row(DIAG, diag)
        row(UP, pick(1) / diag)
        row(DOWN, pick(-1) / diag)
        row(SUM_UP, zs[SUB + depth - 1 : SUB + depth])
        row(SUM_DOWN, zs[SUB : SUB + 1])
        cz = pltpu.roll(cond_ref[:, nx + wy :], lax.rem(wz - z0, wz), 1)
        row(COND, cz)

        lane = lax.broadcasted_iota(jnp.int32, (1, LANES), 1)

        def fill(index, values):
            line = jnp.zeros((1, LANES), f32)
            for at, value in values.items():
                line = jnp.where(lane == at, value, line)
            row(index, line)

        far = total - 1
        core = lax.rem(gy, 2)
        chip = gy // 2
        chips = ny // 2
        yb = chip * (2 * rows)
        one = jnp.ones((1, 1), f32)
        zero = jnp.zeros((1, 1), f32)
        up = over_pivot(ay_ref, yb + 2 * rows - 1, yb + rows - 1)
        down = over_pivot(ay_ref, yb, yb + rows)
        through_up = over_pivot(ay_ref, yb + rows - 1, yb - 1)
        through_down = over_pivot(ay_ref, yb + rows, yb + 2 * rows)
        by_core = lambda a, b: jnp.where(core == 0, a, b)
        fill(
            MISC,
            {
                Z_LOW: zs[SUB : SUB + 1, far:] / zs[SUB - 1 : SUB, far:],
                Z_HIGH: zs[SUB + depth - 1 : SUB + depth, depth : depth + 1]
                / zs[SUB + depth : SUB + depth + 1, depth : depth + 1],
                Y_LOW: ys[SUB - 1 : SUB, :1] / ys[SUB : SUB + 1, :1],
                Y_HIGH: ys[SUB + rows : SUB + rows + 1, rows - 1 : rows]
                / ys[SUB + rows - 1 : SUB + rows, rows - 1 : rows],
                MIX: by_core(up, one),
                MIX + 1: by_core(one, up),
                MIX + 2: by_core(one, down),
                MIX + 3: by_core(down, one),
                KEEP: by_core(one, through_up),
                KEEP + 1: by_core(zero, one),
                KEEP + 2: by_core(through_down, one),
                KEEP + 3: by_core(one, zero),
                GIVE: by_core(through_up, one),
                GIVE + 1: by_core(one, zero),
                GIVE + 2: by_core(one, through_down),
                GIVE + 3: by_core(zero, one),
            },
        )
        values = {}
        for k in range(1, chips):
            src = lax.rem(chip - k + chips, chips)
            below = src < chip
            a = over_pivot(ay_ref, yb - 1, (src + 1) * 2 * rows - 1)
            b = over_pivot(ay_ref, yb + 2 * rows, src * 2 * rows)
            values[k] = jnp.where(below, a, 0.0)
            values[FAR + k] = jnp.where(below, 0.0, b)
        fill(CHIPS, values)
        values = {}
        for k in range(1, nz):
            src = lax.rem(gz - k + nz, nz)
            below = src < gz
            a = over_pivot(az_ref, z0 - 1, (src + 1) * depth - 1)
            b = over_pivot(az_ref, z0 + depth, src * depth)
            values[k] = jnp.where(below, a, 0.0)
            values[FAR + k] = jnp.where(below, 0.0, b)
        fill(LINES, values)


def tables(ids, inverse_x, inverse_y, inverse_z, conds, widths, rows, depth):
    nx = inverse_x.shape[0]
    blocks = nx // XB
    ny, nz = lax.axis_size("gy"), lax.axis_size("gz")
    q, s = XB // LANES, XB // SUB
    column = lambda at: pl.BlockSpec((XB, LANES), lambda e: (e, at(e)))
    low = lambda e: jnp.maximum(q * e - 1, 0)
    top = lambda e: jnp.minimum(q * e + q, q * blocks - 1)
    return call(
        functools.partial(
            tables_kernel, rows=rows, depth=depth, ny=ny, nz=nz, widths=widths
        ),
        [
            shape(blocks, XB, XB, dtype=bf16),
            shape(blocks, XB, XB, dtype=bf16),
            shape(1, nx),
            shape(1, nx),
            shape(4, rows + SUB, LANES),
            shape(2 * rows, 2 * rows, dtype=bf16),
            shape(TABLE_ROWS, LANES),
        ],
        (ids, inverse_x, inverse_x, inverse_x, inverse_x, inverse_x, inverse_y, inverse_z, conds),
        grid=(blocks,),
        in_specs=[
            smem(),
            pl.BlockSpec((XB, XB), lambda e: (e, e)),
            column(low),
            pl.BlockSpec((SUB, LANES), lambda e: (jnp.maximum(s * e - 1, 0), low(e))),
            column(top),
            pl.BlockSpec(
                (SUB, LANES), lambda e: (jnp.minimum(s * e + s, s * blocks - 1), top(e))
            ),
            full(inverse_y), full(inverse_z), full(conds),
        ],
        out_specs=[
            *[VMEM_WHOLE] * 6,
            full(shape(TABLE_ROWS, LANES)),
        ],
        resident=range(6),
        large=2**14,
        name="tables",
    )


def explicit_kernel(
    ids_ref, scal_ref, *rest, nz, resident,
):
    if resident:
        u_ref, *rest = rest
    else:
        u_ref, above_ref, *rest = rest
    o_ref, ylo_ref, yhi_ref, zlo_ref, zhi_ref, cx_ref, wide_ref, *rest = rest
    ay_ref, axh_ref, axl_ref, xlo_ref, xhi_ref, *rest = rest
    t_ref, edge_ref, mine_ref, theirs_ref, *rest = rest
    pays = rest[: nz - 1]
    rhs_ref, line_ref, sy_ref, sz_ref, high_ref, flux_ref = rest[nz - 1 :]
    step = pl.program_id(0)
    steps = pl.num_programs(0)
    zb, rows, nx = o_ref.shape
    tiles = rows // SUB
    blocks = nx // XB
    base_z = step * zb if resident else 0
    sub = lax.broadcasted_iota(jnp.int32, (SUB, nx), 0)
    dot = functools.partial(jnp.dot, preferred_element_type=f32)

    over = u_ref[jnp.minimum(base_z + zb, steps * zb - 1)] if resident else above_ref[0]
    high_ref[...] = jnp.where(step < steps - 1, over, zhi_ref[...])

    @pl.when(step == 0)
    def _():
        sz_ref[...] = jnp.zeros_like(sz_ref)
        flux_ref[...] = (u_ref[0] - zlo_ref[...]) * scal_ref[COND, 0]

    def plane(k, i):
        z = k * PAIR + i
        zz = step * zb + z
        beyond = base_z + jnp.minimum(z + 1, zb - 1)
        c_up = scal_ref[COND, zz + 1]
        cx = jnp.broadcast_to(cx_ref[:, :nx], (SUB, nx))

        def get(r):
            return u_ref[base_z + z, r * SUB : (r + 1) * SUB, :]

        current = get(0)
        first = current[:1] - ylo_ref[pl.ds(zz, 1), :]
        first = first * wide_rows(wide_ref, (3, slice(0, 1)), nx)
        before = jnp.broadcast_to(first, (SUB, nx))
        for r in range(tiles):
            own = slice(r * SUB, (r + 1) * SUB)
            c = current
            if r + 1 < tiles:
                current = get(r + 1)
                up_next = pltpu.roll(current, SUB - 1, 0)
            else:
                up_next = jnp.broadcast_to(yhi_ref[pl.ds(zz, 1), :], (SUB, nx))
            up = jnp.where(sub == SUB - 1, up_next, pltpu.roll(c, SUB - 1, 0))
            fx = (pltpu.roll(c, nx - 1, 1) - c) * cx
            total = fx - pltpu.roll(fx, 1, 1)
            fy = (up - c) * wide_rows(wide_ref, (2, own), nx)
            rolled = pltpu.roll(fy, 1, 0)
            total = total + (fy - jnp.where(sub == 0, before, rolled))
            before = rolled
            above = u_ref[beyond, own, :]
            if i == PAIR - 1:
                above = jnp.where(z == zb - 1, high_ref[own, :], above)
            fz = (above - c) * c_up
            total = total + (fz - flux_ref[own, :])
            flux_ref[own, :] = fz
            o = o_ref[z, own, :]
            total = total + (REACTION * c) * (1.0 - c * c - 2.0 * o)
            rhs_ref[pl.ds(pl.multiple_of(z * rows + r * SUB, SUB), SUB), :] = total

    y_low = scal_ref[MISC, Y_LOW]
    y_high = scal_ref[MISC, Y_HIGH]

    def x_block(e, carry):
        cols = pl.ds(pl.multiple_of(e * XB, XB), XB)
        high, low = split(rhs_ref[:, cols])
        line_ref[:, cols] = (
            dot(high, axh_ref[e]) + dot(low, axh_ref[e]) + dot(high, axl_ref[e])
        )
        return carry

    def y_plane(z, carry):
        zz = step * zb + z
        here = pl.ds(pl.multiple_of(z * rows, rows), rows)
        lows = [None]
        for e in range(blocks - 1):
            at = slice((e + 1) * XB - 1, (e + 1) * XB)
            end = line_ref[here, at]
            if lows[e] is not None:
                end = end + lows[e] * xlo_ref[:, at]
            lows.append(end)
        highs = [None] * blocks
        for e in reversed(range(1, blocks)):
            at = slice(e * XB, e * XB + 1)
            end = line_ref[here, at]
            if highs[e] is not None:
                end = end + highs[e] * xhi_ref[:, at]
            highs[e - 1] = end
        for e in range(blocks):
            cols = slice(e * XB, (e + 1) * XB)
            value = line_ref[here, cols]
            if lows[e] is not None:
                value = value + lows[e] * xlo_ref[:, cols]
            if highs[e] is not None:
                value = value + highs[e] * xhi_ref[:, cols]
            high, low = split(value)
            result = dot(ay_ref[...], jnp.concatenate([high, low], axis=0))
            value = result[:rows] + result[rows:]
            t_ref[zz, :, cols] = value
            bottom, top = value[:1], value[rows - 1 :]
            sy_ref[0, pl.ds(zz, 1), cols] = top
            sy_ref[1, pl.ds(zz, 1), cols] = bottom
            edge_ref[zz, 0:1, cols] = y_low * bottom
            edge_ref[zz, 1:2, cols] = y_high * top
            sz_ref[0, :, cols] = sz_ref[0, :, cols] + scal_ref[SUM_UP, zz] * value
            sz_ref[1, :, cols] = sz_ref[1, :, cols] + scal_ref[SUM_DOWN, zz] * value
        return carry

    def pair(k, carry):
        for i in range(PAIR):
            plane(k, i)
        return carry

    lax.fori_loop(0, zb // PAIR, pair, 0)
    lax.fori_loop(0, blocks, x_block, 0, unroll=True)
    lax.fori_loop(0, zb, y_plane, 0, unroll=YU)

    @pl.when(step == steps - 1)
    def _():
        half = mine_ref.shape[1]
        core = lax.rem(ids_ref[0], 2)
        near = pl.multiple_of(core * half, SUB)
        far = pl.multiple_of((1 - core) * half, SUB)
        mine_ref[...] = sy_ref[:, pl.ds(near, half), :]
        theirs_ref[...] = sy_ref[:, pl.ds(far, half), :]
        for k in range(1, nz):
            higher = ids_ref[1] + k < nz
            pays[k - 1][...] = jnp.where(higher, sz_ref[0], sz_ref[1])


def explicit(ids, scal, u, o, halos, tabs, cx, resident):
    depth, rows, nx = u.shape
    axh, axl, xlo, xhi, wide, mat = tabs
    nz = lax.axis_size("gz")
    zb = ZB
    steps = depth // zb
    half = depth // 2
    field = pl.BlockSpec((zb, rows, nx), lambda s: (s, 0, 0))
    above = pl.BlockSpec(
        (1, rows, nx), lambda s: (jnp.minimum(s * zb + zb, depth - 1), 0, 0)
    )
    rest = (*halos, cx, wide, mat, axh, axl, xlo, xhi)
    outs = [
        shape(depth, rows, nx),
        shape(depth, SUB, nx),
        shape(2, half, nx),
        shape(2, half, nx),
    ] + [shape(rows, nx)] * (nz - 1)
    return call(
        functools.partial(explicit_kernel, nz=nz, resident=resident),
        outs,
        (ids, scal, *([u] if resident else [u, u]), o, *rest),
        grid=(steps,),
        in_specs=[smem(), smem()]
        + ([VMEM_WHOLE] if resident else [field, above])
        + [field, *[VMEM_WHOLE] * 11],
        resident=range(len(outs)),
        out_specs=[VMEM_WHOLE] * len(outs),
        scratch_shapes=[pltpu.VMEM((zb * rows, nx), f32)] * 2
        + [
            pltpu.VMEM((2, depth, nx), f32),
            pltpu.VMEM((2, rows, nx), f32),
            pltpu.VMEM((rows, nx), f32),
            pltpu.VMEM((rows, nx), f32),
        ],
        vmem=VL1,
        name="explicit",
    )


def chip_kernel(ids_ref, scal_ref, mine_ref, other_ref, *pays):
    mix = lambda i: scal_ref[MISC, MIX + i]
    up = mix(0) * mine_ref[0] + mix(1) * other_ref[0]
    down = mix(2) * mine_ref[1] + mix(3) * other_ref[1]
    chip = ids_ref[0] // 2
    for k, pay in enumerate(pays, 1):
        pay[...] = jnp.where(chip + k < len(pays) + 1, up, down)


def share_kernel(scal_ref, mine_ref, other_ref, *rest):
    *gots, keep_ref, give_ref = rest
    low = jnp.zeros_like(gots[0])
    high = jnp.zeros_like(gots[0])
    for k, got in enumerate(gots, 1):
        low = low + scal_ref[CHIPS, k] * got[...]
        high = high + scal_ref[CHIPS, FAR + k] * got[...]
    keep = lambda i: scal_ref[MISC, KEEP + i]
    give = lambda i: scal_ref[MISC, GIVE + i]
    keep_ref[0] = keep(0) * low + keep(1) * other_ref[0]
    keep_ref[1] = keep(2) * high + keep(3) * other_ref[1]
    give_ref[0] = give(0) * low + give(1) * mine_ref[0]
    give_ref[1] = give(2) * high + give(3) * mine_ref[1]


def corner_kernel(ids_ref, scal_ref, keep_ref, back_ref, *pays):
    half = keep_ref.shape[1]
    core = lax.rem(ids_ref[0], 2)
    near, far = core * half, (1 - core) * half
    up = jnp.zeros((2, keep_ref.shape[2]), f32)
    down = jnp.zeros_like(up)
    for z in range(half):
        for ref, base in ((keep_ref, near), (back_ref, far)):
            row = ref[:, z, :]
            up = up + scal_ref[SUM_UP, base + z] * row
            down = down + scal_ref[SUM_DOWN, base + z] * row
    for k, pay in enumerate(pays, 1):
        pay[...] = jnp.where(ids_ref[1] + k < len(pays) + 1, up, down)


def cyclic(size, k, stride=1):
    groups = size // stride
    return [
        (c * stride + r, ((c + k) % groups) * stride + r)
        for c in range(groups)
        for r in range(stride)
    ]


def update_kernel(
    ids_ref, scal_ref, t_ref, u_ref, edge_ref, keep_ref, back_ref, wide_ref,
    ylo_ref, yhi_ref, zlo_ref, zhi_ref, *rest, nz, final, resident,
):
    gots, corners, rest = rest[: nz - 1], rest[nz - 1 : 2 * nz - 2], rest[2 * nz - 2 :]
    if final:
        out_ref, e_ref, pq_ref = rest
    else:
        out_ref, nylo_ref, nyhi_ref, nzlo_ref, nzhi_ref, e_ref, pq_ref, s_ref = rest
    r = pl.program_id(0)
    depth, _, nx = t_ref.shape
    half = keep_ref.shape[1]
    tiles = wide_ref.shape[1] // SUB - 1
    scal = lambda i, j: scal_ref[i, j]

    @pl.when(r == 0)
    def _():
        core = lax.rem(ids_ref[0], 2)
        near = pl.multiple_of(core * half, SUB)
        far = pl.multiple_of((1 - core) * half, SUB)
        pq_ref[:, pl.ds(near, half), :] = keep_ref[...]
        pq_ref[:, pl.ds(far, half), :] = back_ref[...]

    own = pl.ds(pl.multiple_of(r * SUB, SUB), SUB)
    lo = wide_rows(wide_ref, (0, own), nx)
    hi = wide_rows(wide_ref, (1, own), nx)

    def solve(carry_rows, get_t, put_first, put_second):
        low = jnp.zeros((SUB, nx), f32)
        high = jnp.zeros((SUB, nx), f32)
        for k in range(1, nz):
            value = carry_rows(gots[k - 1])
            value = value + lo * corners[k - 1][0:1, :] + hi * corners[k - 1][1:2, :]
            low = low + scal(LINES, k) * value
            high = high + scal(LINES, FAR + k) * value

        def forward(z, carry):
            v = get_t(z) + lo * pq_ref[0, pl.ds(z, 1), :] + hi * pq_ref[1, pl.ds(z, 1), :]
            e = scal(DIAG, z) * v
            e_ref[z] = e
            s = carry + e
            put_first(z, s)
            return scal(UP, z) * s

        above = lax.fori_loop(0, depth, forward, scal(MISC, Z_LOW) * low, unroll=4)

        def backward(k, carry):
            z = depth - 1 - k
            put_second(z, carry)
            return scal(DOWN, z) * (carry + e_ref[z])

        below = lax.fori_loop(0, depth, backward, scal(MISC, Z_HIGH) * high, unroll=4)
        return low + below, high + above

    u_own = own if resident else slice(None)
    out_own = slice(None) if final else own

    def first(z, s):
        out_ref[z, out_own, :] = u_ref[z, u_own, :] + s

    def second(z, b):
        out_ref[z, out_own, :] = out_ref[z, out_own, :] + b

    @pl.when(r < tiles)
    def _():
        below, above = solve(lambda got: got[own, :], lambda z: t_ref[z, own, :], first, second)
        if not final:
            nzlo_ref[own, :] = zlo_ref[own, :] + below
            nzhi_ref[own, :] = zhi_ref[own, :] + above

    if not final:
        y_low = scal(MISC, Y_LOW)
        y_high = scal(MISC, Y_HIGH)
        pad = jnp.zeros((SUB - 2, nx), f32)

        def ends(got):
            rows = got.shape[0]
            return jnp.concatenate(
                [y_low * got[0:1, :], y_high * got[rows - 1 : rows, :], pad], axis=0
            )

        def keep_sum(z, s):
            s_ref[z] = s

        def put(z, b):
            value = s_ref[z] + b
            nylo_ref[pl.ds(z, 1), :] = ylo_ref[pl.ds(z, 1), :] + value[0:1]
            nyhi_ref[pl.ds(z, 1), :] = yhi_ref[pl.ds(z, 1), :] + value[1:2]

        @pl.when(r == tiles)
        def _():
            solve(ends, lambda z: edge_ref[z], keep_sum, put)


def update(ids, scal, t, u, edge, keep, back, wide, halos, gots, corners, final, resident):
    depth, rows, nx = u.shape
    nz = lax.axis_size("gz")
    tiles = rows // SUB
    ylo, yhi, zlo, zhi = halos
    clamp = lambda r: jnp.minimum(r, tiles - 1)
    field = pl.BlockSpec((depth, SUB, nx), lambda r: (0, clamp(r), 0))
    outs = [shape(depth, rows, nx)]
    out_specs = [field] if final else [VMEM_WHOLE] * 5
    scratch = [pltpu.VMEM((depth, SUB, nx), f32), pltpu.VMEM((2, depth, nx), f32)]
    if not final:
        outs += [shape(depth, nx)] * 2 + [shape(rows, nx)] * 2
        scratch += [pltpu.VMEM((depth, SUB, nx), f32)]
    return call(
        functools.partial(update_kernel, nz=nz, final=final, resident=resident),
        outs,
        (ids, scal, t, u, edge, keep, back, wide, ylo, yhi, zlo, zhi, *gots, *corners),
        grid=(tiles if final else tiles + 1,),
        in_specs=[
            smem(), smem(), VMEM_WHOLE, VMEM_WHOLE if resident else field,
            *[VMEM_WHOLE] * (8 + 2 * (nz - 1)),
        ],
        out_specs=out_specs,
        scratch_shapes=scratch,
        resident=() if final else range(5),
        vmem=VL2,
        name="update",
    )


def halo(u):
    ny, nz = lax.axis_size("gy"), lax.axis_size("gz")
    up = lambda n: [(i, i + 1) for i in range(n - 1)]
    down = lambda n: [(i + 1, i) for i in range(n - 1)]
    ylo = lax.ppermute(u[:, -1, :], "gy", up(ny))
    yhi = lax.ppermute(u[:, 0, :], "gy", down(ny))
    zlo = lax.ppermute(u[-1], "gz", cyclic(nz, 1))
    zhi = lax.ppermute(u[0], "gz", cyclic(nz, nz - 1))
    return ylo, yhi, zlo, zhi


def body(phase_field, others, cond_x, cond_y, cond_z, inverse_x, inverse_y, inverse_z):
    depth, rows, nx = phase_field.shape
    ny, nz = lax.axis_size("gy"), lax.axis_size("gz")
    half = depth // 2
    ids = jnp.stack([lax.axis_index("gy"), lax.axis_index("gz")])
    halos = halo(phase_field)
    room = lambda n: -(-(n + 3 + LANES) // LANES) * LANES
    wy, wz = room(cond_y.shape[0]), room(cond_z.shape[0])
    conds = jnp.concatenate(
        [
            jnp.pad(cond_x, (0, 1)),
            jnp.pad(cond_y, (1, wy - 1 - cond_y.shape[0])),
            jnp.pad(cond_z, (1, wz - 1 - cond_z.shape[0])),
        ]
    )[None]
    *tabs, scal = tables(
        ids, inverse_x, inverse_y, inverse_z, conds, (nx, wy, wz), rows, depth
    )
    wide = tabs[4]
    cx = conds
    swap = [(i, i ^ 1) for i in range(ny)]
    u = phase_field
    for step in range(STEPS):
        final = step == STEPS - 1
        t, edge, mine, theirs, *pays = explicit(
            ids, scal, u, others, halos, tabs, cx, step > 0
        )
        gots = []
        for k in range(1, nz):
            gots.append(lax.ppermute(pays[k - 1], "gz", cyclic(nz, k)))
        other = lax.ppermute(theirs, "gy", swap)
        pays = call(
            chip_kernel,
            [shape(half, nx)] * (ny // 2 - 1),
            (ids, scal, mine, other),
            in_specs=[smem(), smem(), VMEM_WHOLE, VMEM_WHOLE],
            out_specs=[VMEM_WHOLE] * (ny // 2 - 1),
            resident=range(ny // 2 - 1),
            name="chip",
        )
        moved = [
            lax.ppermute(pays[k - 1], "gy", cyclic(ny, k, 2))
            for k in range(1, ny // 2)
        ]
        keep, give = call(
            share_kernel,
            [shape(2, half, nx)] * 2,
            (scal, mine, other, *moved),
            in_specs=[smem(), *[VMEM_WHOLE] * (2 + len(moved))],
            out_specs=[VMEM_WHOLE] * 2,
            resident=range(2),
            name="share",
        )
        back = lax.ppermute(give, "gy", swap)
        pays = call(
            corner_kernel,
            [shape(2, nx)] * (nz - 1),
            (ids, scal, keep, back),
            in_specs=[smem(), smem(), VMEM_WHOLE, VMEM_WHOLE],
            out_specs=[VMEM_WHOLE] * (nz - 1),
            resident=range(nz - 1),
            name="corner",
        )
        corners = [lax.ppermute(pays[k - 1], "gz", cyclic(nz, k)) for k in range(1, nz)]
        out = update(
            ids, scal, t, u, edge, keep, back, wide, halos, gots, corners,
            final, step > 0,
        )
        u, halos = out[0], out[1:]
    return u


def solution(mesh):
    placed = (P("gz", "gy", None), P("gz", "gy", None), P(), P(), P(), P(), P(), P())
    return jax.shard_map(
        body, mesh=mesh, in_specs=placed, out_specs=P("gz", "gy", None), check_vma=False
    )
```
